32 devices in a mesh: dp: 4 (over y, x), row: 2 (over core), col: 4 (over z).
Axes of the slice: x: 2, y: 2, z: 4, core: 2. Of those that a mesh axis runs over, the one named last changes fastest.
Arguments:
- inputs: bfloat16 [10240, 1024], P('dp', ('row', 'col')), may hold values from -6 to 6
- positions: int32 [10240], P('dp'), may hold values from 0 to 3837, as said below
- grad_output: bfloat16 [10240, 1024], P('dp', ('row', 'col')), may hold values from -6 to 6
- ffn1_norm_gain: bfloat16 [1024], P(('row', 'col')), may hold values from 0.5 to 1.5
- ffn1_norm_shift: bfloat16 [1024], P(('row', 'col')), may hold values from -1.5 to 1.5
- ffn1_in: bfloat16 [1024, 4096], P('row', 'col'), may hold values from -0.1875 to 0.1875
- ffn1_in_bias: bfloat16 [4096], replicated, may hold values from -1.5 to 1.5
- ffn1_out: bfloat16 [4096, 1024], P('col', 'row'), may hold values from -0.09375 to 0.09375
- ffn1_out_bias: bfloat16 [1024], P(('row', 'col')), may hold values from -1.5 to 1.5
- attn_norm_gain: bfloat16 [1024], P(('row', 'col')), may hold values from 0.5 to 1.5
- attn_norm_shift: bfloat16 [1024], P(('row', 'col')), may hold values from -1.5 to 1.5
- query_weight: bfloat16 [1024, 1024], P('row', 'col'), may hold values from -0.1875 to 0.1875
- query_bias: bfloat16 [1024], replicated, may hold values from -1.5 to 1.5
- key_weight: bfloat16 [1024, 1024], P('row', 'col'), may hold values from -0.1875 to 0.1875
- value_weight: bfloat16 [1024, 1024], P('row', 'col'), may hold values from -0.1875 to 0.1875
- value_bias: bfloat16 [1024], replicated, may hold values from -1.5 to 1.5
- distance_table: bfloat16 [73, 64], replicated, may hold values from -5 to 5
- attn_out: bfloat16 [1024, 1024], P('col', 'row'), may hold values from -0.75 to 0.75
- attn_out_bias: bfloat16 [1024], P(('row', 'col')), may hold values from -1.5 to 1.5
- conv_norm_gain: bfloat16 [1024], P(('row', 'col')), may hold values from 0.5 to 1.5
- conv_norm_shift: bfloat16 [1024], P(('row', 'col')), may hold values from -1.5 to 1.5
- glu_value: bfloat16 [1024, 1024], P('row', 'col'), may hold values from -0.1875 to 0.1875
- glu_gate: bfloat16 [1024, 1024], P('row', 'col'), may hold values from -0.1875 to 0.1875
- depth_kernel: bfloat16 [31, 1024], replicated, may hold values from -1 to 1
- depth_norm_gain: bfloat16 [1024], replicated, may hold values from 0.5 to 1.5
- depth_norm_shift: bfloat16 [1024], replicated, may hold values from -1.5 to 1.5
- conv_out: bfloat16 [1024, 1024], P('col', 'row'), may hold values from -0.1875 to 0.1875
- ffn2_norm_gain: bfloat16 [1024], P(('row', 'col')), may hold values from 0.5 to 1.5
- ffn2_norm_shift: bfloat16 [1024], P(('row', 'col')), may hold values from -1.5 to 1.5
- ffn2_in: bfloat16 [1024, 4096], P('row', 'col'), may hold values from -0.1875 to 0.1875
- ffn2_in_bias: bfloat16 [4096], replicated, may hold values from -1.5 to 1.5
- ffn2_out: bfloat16 [4096, 1024], P('col', 'row'), may hold values from -0.09375 to 0.09375
- ffn2_out_bias: bfloat16 [1024], P(('row', 'col')), may hold values from -1.5 to 1.5
- final_norm_gain: bfloat16 [1024], P(('row', 'col')), may hold values from 0.5 to 1.5
- final_norm_shift: bfloat16 [1024], P(('row', 'col')), may hold values from -1.5 to 1.5
Outputs:
- output: bfloat16 [10240, 1024], P('dp', ('row', 'col'))
- input_grad: float32 [10240, 1024], P('dp', ('row', 'col'))
- ffn1_norm_gain_grad: float32 [1024], P(('row', 'col'))
- ffn1_norm_shift_grad: float32 [1024], P(('row', 'col'))
- ffn1_in_grad: float32 [1024, 4096], P('row', 'col')
- ffn1_in_bias_grad: float32 [4096], replicated
- ffn1_out_grad: float32 [4096, 1024], P('col', 'row')
- ffn1_out_bias_grad: float32 [1024], P(('row', 'col'))
- attn_norm_gain_grad: float32 [1024], P(('row', 'col'))
- attn_norm_shift_grad: float32 [1024], P(('row', 'col'))
- query_weight_grad: float32 [1024, 1024], P('row', 'col')
- query_bias_grad: float32 [1024], replicated
- key_weight_grad: float32 [1024, 1024], P('row', 'col')
- value_weight_grad: float32 [1024, 1024], P('row', 'col')
- value_bias_grad: float32 [1024], replicated
- distance_table_grad: float32 [73, 64], replicated
- attn_out_grad: float32 [1024, 1024], P('col', 'row')
- attn_out_bias_grad: float32 [1024], P(('row', 'col'))
- conv_norm_gain_grad: float32 [1024], P(('row', 'col'))
- conv_norm_shift_grad: float32 [1024], P(('row', 'col'))
- glu_value_grad: float32 [1024, 1024], P('row', 'col')
- glu_gate_grad: float32 [1024, 1024], P('row', 'col')
- depth_kernel_grad: float32 [31, 1024], replicated
- depth_norm_gain_grad: float32 [1024], replicated
- depth_norm_shift_grad: float32 [1024], replicated
- conv_out_grad: float32 [1024, 1024], P('col', 'row')
- ffn2_norm_gain_grad: float32 [1024], P(('row', 'col'))
- ffn2_norm_shift_grad: float32 [1024], P(('row', 'col'))
- ffn2_in_grad: float32 [1024, 4096], P('row', 'col')
- ffn2_in_bias_grad: float32 [4096], replicated
- ffn2_out_grad: float32 [4096, 1024], P('col', 'row')
- ffn2_out_bias_grad: float32 [1024], P(('row', 'col'))
- final_norm_gain_grad: float32 [1024], P(('row', 'col'))
- final_norm_shift_grad: float32 [1024], P(('row', 'col'))
The draws below stay inside these ranges and needn't reach their ends.
Inputs may be any that keep to these rules, and one draw needn't show every extreme that they name: Within each clip of 1280 tokens the positions start at 0 and rise by 1 to 3 from one token to the next; in the first clip every rise is 3.
All inputs are finite; a program needn't handle non-finite values.
Results may differ from the reference program's by a relative error of at most 0.025.
Values may be sent and summed in bfloat16 or wider, within the bound.
A program may use at most 320 MiB of HBM per device.

```python
import jax
import jax.numpy as jnp
from jax import lax

D = 1024
HEADS = 16
HEAD = 64
FF = 4096
KERNEL = 31
LEFT = 64
RIGHT = 8
L = 1280
CLIPS_MB = 1
BUCKETS = 73
TOKENS = 10240


def draw_positions(key, part):
    steps_drawn = jax.random.randint(key, (TOKENS // L, L), 1, 4)
    first_clip = jnp.arange(TOKENS // L)[:, None] == 0
    steps_drawn = jnp.where(first_clip, 3, steps_drawn)
    first_col = jnp.arange(L)[None, :] == 0
    steps_drawn = jnp.where(first_col, 0, steps_drawn)
    return jnp.cumsum(steps_drawn, axis=1).reshape(TOKENS).astype(jnp.int32)


def shard_levels(own_key, extent, split, least, top_value):
    level, own = 1.0, jax.random.fold_in(own_key, 6)
    for dim, blocks in split:
        draws = jnp.exp(jax.random.uniform(jax.random.fold_in(own, dim), (blocks,), jnp.float32, least / len(split), top_value / len(split)))
        level = level * jnp.repeat(draws, extent[dim] // blocks).reshape([-1 if axis == dim else 1 for axis in range(len(extent))])
    return level


def bell_draw(key, extent, scale, bound, pieces=(), kind=jnp.bfloat16):
    array = jax.random.normal(key, extent, jnp.float32) * scale
    if len(pieces) > 0:
        array = shard_levels(key, extent, pieces, -0.22, 0.18) * array
    return jnp.clip(array, min=-bound, max=bound).astype(kind)


def setup_inputs(seed: int = 0) -> dict:
    keys = jax.random.split(jax.random.key(seed), 36)
    inputs = bell_draw(keys[0], (TOKENS, D), 1.0, 6.0, ((0, 4), (1, 8)))
    positions = draw_positions(jax.random.fold_in(keys[35], 71), 0)
    grad_output = bell_draw(keys[2], (TOKENS, D), 1.0, 6.0, ((0, 4), (1, 8)))
    ffn1_norm_gain = jnp.clip(1.0 + 0.1 * jax.random.normal(keys[3], (D,), jnp.float32), 0.5, 1.5).astype(jnp.bfloat16)
    ffn1_norm_shift = bell_draw(keys[4], (D,), 0.3, 1.5, ((0, 8),))
    ffn1_in = bell_draw(keys[5], (D, FF), D ** -0.5, 0.1875, ((0, 2), (1, 4)))
    ffn1_in_bias = bell_draw(keys[6], (FF,), 0.3, 1.5)
    ffn1_out = bell_draw(keys[7], (FF, D), FF ** -0.5, 0.09375, ((0, 4), (1, 2)))
    ffn1_out_bias = bell_draw(keys[8], (D,), 0.3, 1.5, ((0, 8),))
    attn_norm_gain = jnp.clip(1.0 + 0.1 * jax.random.normal(keys[9], (D,), jnp.float32), 0.5, 1.5).astype(jnp.bfloat16)
    attn_norm_shift = bell_draw(keys[10], (D,), 0.3, 1.5, ((0, 8),))
    query_weight = bell_draw(keys[11], (D, D), D ** -0.5, 0.1875, ((0, 2), (1, 4)))
    query_bias = bell_draw(keys[12], (D,), 0.3, 1.5)
    key_weight = bell_draw(keys[13], (D, D), D ** -0.5, 0.1875, ((0, 2), (1, 4)))
    value_weight = bell_draw(keys[14], (D, D), D ** -0.5, 0.1875, ((0, 2), (1, 4)))
    value_bias = bell_draw(keys[15], (D,), 0.3, 1.5)
    distance_table = bell_draw(keys[16], (BUCKETS, HEAD), 1.0, 5.0)
    attn_out = bell_draw(keys[17], (D, D), (D // 16) ** -0.5, 0.75, ((0, 4), (1, 2)))
    attn_out_bias = bell_draw(keys[18], (D,), 0.3, 1.5, ((0, 8),))
    conv_norm_gain = jnp.clip(1.0 + 0.1 * jax.random.normal(keys[19], (D,), jnp.float32), 0.5, 1.5).astype(jnp.bfloat16)
    conv_norm_shift = bell_draw(keys[20], (D,), 0.3, 1.5, ((0, 8),))
    glu_value = bell_draw(keys[21], (D, D), D ** -0.5, 0.1875, ((0, 2), (1, 4)))
    glu_gate = bell_draw(keys[22], (D, D), D ** -0.5, 0.1875, ((0, 2), (1, 4)))
    depth_kernel = bell_draw(keys[23], (KERNEL, D), KERNEL ** -0.5, 1.0)
    depth_norm_gain = jnp.clip(1.0 + 0.1 * jax.random.normal(keys[24], (D,), jnp.float32), 0.5, 1.5).astype(jnp.bfloat16)
    depth_norm_shift = bell_draw(keys[25], (D,), 0.3, 1.5)
    conv_out = bell_draw(keys[26], (D, D), D ** -0.5, 0.1875, ((0, 4), (1, 2)))
    ffn2_norm_gain = jnp.clip(1.0 + 0.1 * jax.random.normal(keys[27], (D,), jnp.float32), 0.5, 1.5).astype(jnp.bfloat16)
    ffn2_norm_shift = bell_draw(keys[28], (D,), 0.3, 1.5, ((0, 8),))
    ffn2_in = bell_draw(keys[29], (D, FF), D ** -0.5, 0.1875, ((0, 2), (1, 4)))
    ffn2_in_bias = bell_draw(keys[30], (FF,), 0.3, 1.5)
    ffn2_out = bell_draw(keys[31], (FF, D), FF ** -0.5, 0.09375, ((0, 4), (1, 2)))
    ffn2_out_bias = bell_draw(keys[32], (D,), 0.3, 1.5, ((0, 8),))
    final_norm_gain = jnp.clip(1.0 + 0.1 * jax.random.normal(keys[33], (D,), jnp.float32), 0.5, 1.5).astype(jnp.bfloat16)
    final_norm_shift = bell_draw(keys[34], (D,), 0.3, 1.5, ((0, 8),))
    return {"inputs": inputs, "positions": positions, "grad_output": grad_output, "ffn1_norm_gain": ffn1_norm_gain, "ffn1_norm_shift": ffn1_norm_shift, "ffn1_in": ffn1_in, "ffn1_in_bias": ffn1_in_bias, "ffn1_out": ffn1_out, "ffn1_out_bias": ffn1_out_bias, "attn_norm_gain": attn_norm_gain, "attn_norm_shift": attn_norm_shift, "query_weight": query_weight, "query_bias": query_bias, "key_weight": key_weight, "value_weight": value_weight, "value_bias": value_bias, "distance_table": distance_table, "attn_out": attn_out, "attn_out_bias": attn_out_bias, "conv_norm_gain": conv_norm_gain, "conv_norm_shift": conv_norm_shift, "glu_value": glu_value, "glu_gate": glu_gate, "depth_kernel": depth_kernel, "depth_norm_gain": depth_norm_gain, "depth_norm_shift": depth_norm_shift, "conv_out": conv_out, "ffn2_norm_gain": ffn2_norm_gain, "ffn2_norm_shift": ffn2_norm_shift, "ffn2_in": ffn2_in, "ffn2_in_bias": ffn2_in_bias, "ffn2_out": ffn2_out, "ffn2_out_bias": ffn2_out_bias, "final_norm_gain": final_norm_gain, "final_norm_shift": final_norm_shift}


EPSILON = 1e-05
HIGHEST = lax.Precision.HIGHEST

@jax.custom_vjp
def low(v):
    return lax.optimization_barrier(v.astype(jnp.bfloat16)).astype(jnp.float32)

@jax.custom_vjp
def low_back(v):
    return v

def low_keep(v):
    return (low(v), None)

def low_pass(kept, grad):
    return (grad,)

def back_keep(v):
    return (v, None)

def back_low(kept, grad):
    return (low(grad),)
low.defvjp(low_keep, low_pass)
low_back.defvjp(back_keep, back_low)

def layer_norm(values, norm_gain, norm_shift):
    mean_value = lax.optimization_barrier(jnp.mean(values, axis=-1, keepdims=True))
    second = lax.optimization_barrier(jnp.mean(values * values, axis=-1, keepdims=True)) - mean_value * mean_value
    return (values - mean_value) * lax.rsqrt(second + EPSILON) * norm_gain + norm_shift

def matmul(left, right):
    return jnp.dot(left, right, precision=HIGHEST)

def swish_act(values):
    return values * jax.nn.sigmoid(values)

def feed_forward(stream, norm_gain, norm_shift, w_in, b_in, w_out, b_out):
    normed = low(layer_norm(stream, norm_gain, norm_shift))
    hidden = low(swish_act(low_back(matmul(normed, w_in) + b_in)))
    return low_back(matmul(hidden, w_out) + b_out)

def attend_clip(queries, key_rows, values, places, distance):
    bucket = jnp.clip(places[None, :] - places[:, None], -LEFT, RIGHT) + LEFT
    direct = jnp.einsum('qhd,khd->hqk', queries, key_rows, precision=HIGHEST)
    toward = jnp.einsum('qhd,bd->hqb', queries, distance, precision=HIGHEST)
    picked = jnp.take_along_axis(toward, jnp.broadcast_to(bucket[None], direct.shape), axis=2)
    scores = low_back((direct + picked) * HEAD ** (-0.5))
    weights = jax.nn.softmax(scores, axis=-1)
    return jnp.einsum('hqk,khd->qhd', low(weights), values, precision=HIGHEST)

def attention(stream, places, norm_gain, norm_shift, w_query, b_query, w_key, w_value, b_value, distance, w_out, b_out):
    normed = low(layer_norm(stream, norm_gain, norm_shift))
    queries = low(low_back(matmul(normed, w_query) + b_query))
    key_rows = low(low_back(matmul(normed, w_key)))
    values = low(low_back(matmul(normed, w_value) + b_value))
    clip_count = stream.shape[0] // L
    clip_step = jax.checkpoint(attend_clip)

    def one_clip(map_item):
        return clip_step(map_item[0], map_item[1], map_item[2], map_item[3], distance)
    mixed_rows = lax.map(one_clip, (queries.reshape(clip_count, L, HEADS, HEAD), key_rows.reshape(clip_count, L, HEADS, HEAD), values.reshape(clip_count, L, HEADS, HEAD), places.reshape(clip_count, L)))
    mixed_rows = low(low_back(mixed_rows.reshape(stream.shape[0], D)))
    return low_back(matmul(mixed_rows, w_out) + b_out)

def convolution(stream, norm_gain, norm_shift, w_value, w_gate, kernel, depth_gain, depth_shift, w_out):
    normed = low(layer_norm(stream, norm_gain, norm_shift))
    value_part = low_back(matmul(normed, w_value))
    gate_part = low_back(matmul(normed, w_gate))
    mixed_rows = (value_part * jax.nn.sigmoid(gate_part)).reshape(-1, L, D)
    padded = jnp.pad(mixed_rows, ((0, 0), (KERNEL - 1, 0), (0, 0)))
    depth_out = kernel[0] * padded[:, 0:L]
    for tap_index in range(1, KERNEL):
        depth_out = depth_out + kernel[tap_index] * padded[:, tap_index:tap_index + L]
    activated = low(swish_act(layer_norm(depth_out.reshape(-1, D), depth_gain, depth_shift)))
    return low_back(matmul(activated, w_out))

def conformer_layer(stream, places, params):
    stream = stream + 0.5 * feed_forward(stream, params[0], params[1], params[2], params[3], params[4], params[5])
    stream = stream + attention(stream, places, params[6], params[7], params[8], params[9], params[10], params[11], params[12], params[13], params[14], params[15])
    stream = stream + convolution(stream, params[16], params[17], params[18], params[19], params[20], params[21], params[22], params[23])
    stream = stream + 0.5 * feed_forward(stream, params[24], params[25], params[26], params[27], params[28], params[29])
    return layer_norm(stream, params[30], params[31])

def reference(inputs, positions, grad_output, ffn1_norm_gain, ffn1_norm_shift, ffn1_in, ffn1_in_bias, ffn1_out, ffn1_out_bias, attn_norm_gain, attn_norm_shift, query_weight, query_bias, key_weight, value_weight, value_bias, distance_table, attn_out, attn_out_bias, conv_norm_gain, conv_norm_shift, glu_value, glu_gate, depth_kernel, depth_norm_gain, depth_norm_shift, conv_out, ffn2_norm_gain, ffn2_norm_shift, ffn2_in, ffn2_in_bias, ffn2_out, ffn2_out_bias, final_norm_gain, final_norm_shift):
    params = tuple((entry.astype(jnp.float32) for entry in (ffn1_norm_gain, ffn1_norm_shift, ffn1_in, ffn1_in_bias, ffn1_out, ffn1_out_bias, attn_norm_gain, attn_norm_shift, query_weight, query_bias, key_weight, value_weight, value_bias, distance_table, attn_out, attn_out_bias, conv_norm_gain, conv_norm_shift, glu_value, glu_gate, depth_kernel, depth_norm_gain, depth_norm_shift, conv_out, ffn2_norm_gain, ffn2_norm_shift, ffn2_in, ffn2_in_bias, ffn2_out, ffn2_out_bias, final_norm_gain, final_norm_shift)))
    group_rows = CLIPS_MB * L
    group_count = TOKENS // group_rows
    streams = inputs.astype(jnp.float32).reshape(group_count, group_rows, D)
    places = positions.reshape(group_count, group_rows)
    layer_step = jax.checkpoint(conformer_layer)

    def whole_layer(weights, states):
        return lax.map(lambda map_item: layer_step(map_item[0], map_item[1], weights), (states, places))
    result, pullback = jax.vjp(whole_layer, params, streams)
    weight_grads, stream_grad = pullback(grad_output.astype(jnp.float32).reshape(group_count, group_rows, D))
    return (result.reshape(TOKENS, D).astype(jnp.bfloat16), stream_grad.reshape(TOKENS, D), weight_grads[0], weight_grads[1], weight_grads[2], weight_grads[3], weight_grads[4], weight_grads[5], weight_grads[6], weight_grads[7], weight_grads[8], weight_grads[9], weight_grads[10], weight_grads[11], weight_grads[12], weight_grads[13], weight_grads[14], weight_grads[15], weight_grads[16], weight_grads[17], weight_grads[18], weight_grads[19], weight_grads[20], weight_grads[21], weight_grads[22], weight_grads[23], weight_grads[24], weight_grads[25], weight_grads[26], weight_grads[27], weight_grads[28], weight_grads[29], weight_grads[30], weight_grads[31])
```

```python
import functools

import jax
import jax.numpy as jnp
from jax import lax
from jax.experimental import pallas as pl
from jax.experimental.pallas import tpu as pltpu
from jax.sharding import PartitionSpec as P

D = 1024
HEAD = 64
FF = 4096
KERNEL = 31
LEFT = 64
RIGHT = 8
L = 1280
BUCKETS = LEFT + RIGHT + 1
EPSILON = 1e-05
SCALE = HEAD ** (-0.5)
LANES = 128
TQ = 256
EDGE = 128
WINDOW = TQ + 2 * EDGE
F32 = jnp.float32
BF16 = jnp.bfloat16
MESH = pl.DeviceIdType.MESH


def chunk_index():
    return lax.axis_index("col") * lax.axis_size("row") + lax.axis_index("row")


def exchange_kernel(count, members, rows, feature_order, to_cols, *refs):
    sources = refs[:count]
    targets = refs[count : 2 * count]
    send_sem, recv_sem, own_sem = refs[2 * count :]
    row_size = lax.axis_size("row")
    col_size = lax.axis_size("col")
    me = lax.axis_index("col") * row_size + lax.axis_index("row")
    member = lax.rem(me, members)
    base = me - member

    def place(index):
        return {"row": lax.rem(index, row_size), "col": lax.div(index, row_size)}

    def column_of(index):
        if feature_order:
            return lax.rem(index, row_size) * col_size + lax.div(index, row_size)
        return lax.rem(index, members)

    def views(number, peer, peer_member):
        source, target = sources[number], targets[number]
        if to_cols:
            width = source.shape[1]
            return (
                source.at[pl.ds(pl.multiple_of(peer_member * rows, rows), rows), :],
                target.at[:, pl.ds(pl.multiple_of(column_of(me) * width, width), width)],
            )
        width = target.shape[1]
        return (
            source.at[:, pl.ds(pl.multiple_of(column_of(peer) * width, width), width)],
            target.at[pl.ds(pl.multiple_of(member * rows, rows), rows), :],
        )

    barrier = pltpu.get_barrier_semaphore()
    peers = []
    for step in range(1, members):
        peer_member = lax.rem(member + step, members)
        peers.append((base + peer_member, peer_member))
    for peer, unused in peers:
        pl.semaphore_signal(barrier, inc=1, device_id=place(peer), device_id_type=MESH)
    pl.semaphore_wait(barrier, members - 1)
    copies = []
    for step, (peer, peer_member) in enumerate(peers):
        for number in range(count):
            source, target = views(number, peer, peer_member)
            copy = pltpu.make_async_remote_copy(
                src_ref=source,
                dst_ref=target,
                send_sem=send_sem.at[step * count + number],
                recv_sem=recv_sem.at[step * count + number],
                device_id=place(peer),
                device_id_type=MESH,
            )
            copy.start()
            copies.append(copy)
    for number in range(count):
        source, target = views(number, me, member)
        copy = pltpu.make_async_copy(source, target, own_sem.at[number])
        copy.start()
        copies.append(copy)
    for copy in copies:
        copy.wait()


def narrow_exchange(array, members, to_cols):
    if to_cols:
        rows = array.shape[0] // members
        full = lax.all_gather(array, ("row", "col"), axis=1, tiled=True)
        return lax.dynamic_slice_in_dim(full, chunk_index() * rows, rows, 0)
    width = array.shape[1] // members
    full = lax.all_gather(array, ("col", "row"), axis=0, tiled=True)
    column = lax.axis_index("row") * lax.axis_size("col") + lax.axis_index("col")
    return lax.dynamic_slice_in_dim(full, column * width, width, 1)


def exchange(arrays, members, to_cols, call_id, feature_order=False):
    count = len(arrays)
    if feature_order and D // members < LANES:
        return [narrow_exchange(array, members, to_cols) for array in arrays]
    shapes = []
    for array in arrays:
        height, width = array.shape
        if to_cols:
            rows = height // members
            shapes.append(jax.ShapeDtypeStruct((rows, width * members), array.dtype))
        else:
            rows = height
            shapes.append(jax.ShapeDtypeStruct((height * members, width // members), array.dtype))
    any_spec = pl.BlockSpec(memory_space=pl.ANY)
    return pl.pallas_call(
        functools.partial(exchange_kernel, count, members, rows, feature_order, to_cols),
        out_shape=shapes,
        in_specs=[any_spec] * count,
        out_specs=[any_spec] * count,
        scratch_shapes=[
            pltpu.SemaphoreType.DMA(((members - 1) * count,)),
            pltpu.SemaphoreType.DMA(((members - 1) * count,)),
            pltpu.SemaphoreType.DMA((count,)),
        ],
        compiler_params=pltpu.CompilerParams(collective_id=call_id, has_side_effects=True),
    )(*arrays)


def contract(left, right, left_dim, right_dim):
    return lax.dot_general(
        left, right, (((left_dim,), (right_dim,)), ((), ())), preferred_element_type=F32
    )


def head_of(ref, head):
    return ref[:, head * HEAD : (head + 1) * HEAD]


def biased_scores(query, key_rows, table, buckets, row_start, score_ref):
    toward = contract(query, table, 1, 1)
    columns = lax.broadcasted_iota(jnp.int32, (1, L), 1)
    outer = jnp.where(
        columns < row_start - EDGE,
        toward[:, 0:1],
        jnp.where(columns < row_start + TQ + EDGE, 0.0, toward[:, BUCKETS - 1 : BUCKETS]),
    )
    score_ref[:, EDGE : EDGE + L] = contract(query, key_rows, 1, 1) + outer
    for block in range(WINDOW // LANES):
        lanes = pl.ds(pl.multiple_of(row_start + block * LANES, LANES), LANES)
        picked = jnp.take_along_axis(
            toward, buckets[:, block * LANES : (block + 1) * LANES], axis=1
        )
        score_ref[:, lanes] = score_ref[:, lanes] + picked
    return score_ref[:, EDGE : EDGE + L] * SCALE


def window_buckets(place_ref, wide_ref, row_start):
    lanes = pl.ds(pl.multiple_of(row_start, LANES), WINDOW)
    return jnp.clip(wide_ref[:, lanes] - place_ref[...], -LEFT, RIGHT) + LEFT


def attend_kernel(q_ref, k_ref, v_ref, table_ref, place_ref, wide_ref, o_ref, lse_ref, score_ref):
    row_start = pl.program_id(0) * TQ
    buckets = window_buckets(place_ref, wide_ref, row_start)
    table = table_ref[...]
    head_count = q_ref.shape[1] // HEAD
    parts = []
    sums = []
    for head in range(head_count):
        scores = biased_scores(
            head_of(q_ref, head), head_of(k_ref, head), table, buckets, row_start, score_ref
        )
        row_max = jnp.max(scores, axis=1, keepdims=True)
        weights = jnp.exp(scores - row_max)
        total = jnp.sum(weights, axis=1, keepdims=True)
        low = (weights * (1.0 / total)).astype(BF16)
        parts.append(contract(low, head_of(v_ref, head), 1, 0).astype(BF16))
        sums.append(row_max + jnp.log(total))
    o_ref[...] = jnp.concatenate(parts, axis=1)
    lse_ref[...] = jnp.concatenate(sums, axis=1)


def split_low(values):
    high = values.astype(BF16)
    return high, (values - high.astype(F32)).astype(BF16)


def attend_back_kernel(
    q_ref,
    k_ref,
    v_ref,
    go_ref,
    lse_ref,
    table_ref,
    place_ref,
    wide_ref,
    inverse_ref,
    gq_ref,
    gk_ref,
    gv_ref,
    gt_ref,
    score_ref,
    gk_sum,
    gv_sum,
):
    step = pl.program_id(0)
    row_start = step * TQ
    buckets = window_buckets(place_ref, wide_ref, row_start)
    table = table_ref[...]
    inverse = inverse_ref[...] - (row_start - EDGE)
    offsets = wide_ref[:, EDGE : EDGE + L] - place_ref[...]
    low_edge = offsets <= -LEFT
    high_edge = offsets >= RIGHT
    bucket_lane = lax.broadcasted_iota(jnp.int32, (TQ, LANES), 1)
    head_count = q_ref.shape[1] // HEAD

    @pl.when(step == 0)
    def clear():
        gk_sum[...] = jnp.zeros_like(gk_sum)
        gv_sum[...] = jnp.zeros_like(gv_sum)
        gt_ref[...] = jnp.zeros_like(gt_ref)

    gq_parts = []
    gk_parts = []
    gv_parts = []
    table_grad = jnp.zeros((LANES, HEAD), F32)
    for head in range(head_count):
        query = head_of(q_ref, head)
        key_rows = head_of(k_ref, head)
        grad = head_of(go_ref, head)
        scores = biased_scores(query, key_rows, table, buckets, row_start, score_ref)
        probs = jnp.exp(scores - lse_ref[:, head : head + 1])
        prob_grad = contract(grad, head_of(v_ref, head), 1, 1)
        inner = jnp.sum(probs * prob_grad, axis=1, keepdims=True)
        score_grad = (probs * (prob_grad - inner)).astype(BF16)
        gv_parts.append(contract(probs.astype(BF16), grad, 0, 0))
        gk_parts.append(contract(score_grad, query, 0, 0) * SCALE)
        wide_grad = score_grad.astype(F32)
        low_total = jnp.sum(jnp.where(low_edge, wide_grad, 0.0), axis=1, keepdims=True)
        high_total = jnp.sum(jnp.where(high_edge, wide_grad, 0.0), axis=1, keepdims=True)
        score_ref[:, EDGE : EDGE + L] = wide_grad
        spread = jnp.where(
            bucket_lane == 0, low_total, jnp.where(bucket_lane == BUCKETS - 1, high_total, 0.0)
        )
        for block in range(WINDOW // LANES):
            lanes = pl.ds(pl.multiple_of(row_start + block * LANES, LANES), LANES)
            local = inverse - block * LANES
            inside = (local >= 0) & (local < LANES)
            picked = jnp.take_along_axis(
                score_ref[:, lanes], jnp.clip(local, 0, LANES - 1), axis=1
            )
            spread = spread + jnp.where(inside, picked, 0.0)
        spread_high, spread_low = split_low(spread)
        gq_parts.append(
            (
                (
                    contract(score_grad, key_rows, 1, 0)
                    + (contract(spread_high, table, 1, 0) + contract(spread_low, table, 1, 0))
                )
                * SCALE
            ).astype(BF16)
        )
        table_grad = table_grad + (
            contract(spread_high, query, 0, 0) + contract(spread_low, query, 0, 0)
        )
    gq_ref[...] = jnp.concatenate(gq_parts, axis=1)
    gk_sum[...] += jnp.concatenate(gk_parts, axis=1)
    gv_sum[...] += jnp.concatenate(gv_parts, axis=1)
    gt_ref[...] += table_grad * SCALE

    @pl.when(step == pl.num_programs(0) - 1)
    def flush():
        gk_ref[...] = gk_sum[...].astype(BF16)
        gv_ref[...] = gv_sum[...].astype(BF16)


def clip_places(places):
    wide = jnp.pad(places, (EDGE, EDGE))
    column = places[:, None]
    band = jnp.stack(
        [wide[EDGE - LEFT + 1 + o : EDGE - LEFT + 1 + o + L] for o in range(LEFT + RIGHT - 1)],
        axis=1,
    )
    row_index = jnp.arange(L, dtype=jnp.int32)[:, None, None]
    shift = jnp.arange(LEFT + RIGHT - 1, dtype=jnp.int32)[None, :, None]
    key_index = row_index + shift - (LEFT - 1)
    bucket = jnp.arange(LANES, dtype=jnp.int32)
    bucket = jnp.where((bucket > 0) & (bucket < BUCKETS - 1), bucket, 1 << 20)[None, None, :]
    match = (
        (band[:, :, None] == column[:, :, None] + (bucket - LEFT))
        & (key_index >= 0)
        & (key_index < L)
    )
    inverse = jnp.sum(jnp.where(match, key_index + 1 + WINDOW * 8, 0), axis=1) - 1 - WINDOW * 8
    return column, wide[None, :], inverse


def attend(queries, key_rows, values, table, column, wide):
    width = queries.shape[1]
    head_count = width // HEAD
    tile = pl.BlockSpec((TQ, width), lambda i: (i, 0))
    whole = pl.BlockSpec((L, width), lambda i: (0, 0))
    return pl.pallas_call(
        attend_kernel,
        grid=(L // TQ,),
        out_shape=[
            jax.ShapeDtypeStruct((L, width), BF16),
            jax.ShapeDtypeStruct((L, head_count), F32),
        ],
        in_specs=[
            tile,
            whole,
            whole,
            pl.BlockSpec((LANES, HEAD), lambda i: (0, 0)),
            pl.BlockSpec((TQ, 1), lambda i: (i, 0)),
            pl.BlockSpec((1, L + 2 * EDGE), lambda i: (0, 0)),
        ],
        out_specs=[tile, pl.BlockSpec((TQ, head_count), lambda i: (i, 0))],
        scratch_shapes=[pltpu.VMEM((TQ, L + 2 * EDGE), F32)],
        cost_estimate=pl.CostEstimate(
            flops=4 * L * L * width, bytes_accessed=8 * L * width, transcendentals=L * L * head_count
        ),
    )(queries, key_rows, values, table, column, wide)


def attend_back(queries, key_rows, values, grad, lse, table, column, wide, inverse):
    width = queries.shape[1]
    head_count = width // HEAD
    tile = pl.BlockSpec((TQ, width), lambda i: (i, 0))
    whole = pl.BlockSpec((L, width), lambda i: (0, 0))
    return pl.pallas_call(
        attend_back_kernel,
        grid=(L // TQ,),
        out_shape=[
            jax.ShapeDtypeStruct((L, width), BF16),
            jax.ShapeDtypeStruct((L, width), BF16),
            jax.ShapeDtypeStruct((L, width), BF16),
            jax.ShapeDtypeStruct((LANES, HEAD), F32),
        ],
        in_specs=[
            tile,
            whole,
            whole,
            tile,
            pl.BlockSpec((TQ, head_count), lambda i: (i, 0)),
            pl.BlockSpec((LANES, HEAD), lambda i: (0, 0)),
            pl.BlockSpec((TQ, 1), lambda i: (i, 0)),
            pl.BlockSpec((1, L + 2 * EDGE), lambda i: (0, 0)),
            pl.BlockSpec((TQ, LANES), lambda i: (i, 0)),
        ],
        out_specs=[tile, whole, whole, pl.BlockSpec((LANES, HEAD), lambda i: (0, 0))],
        scratch_shapes=[
            pltpu.VMEM((TQ, L + 2 * EDGE), F32),
            pltpu.VMEM((L, width), F32),
            pltpu.VMEM((L, width), F32),
        ],
        cost_estimate=pl.CostEstimate(
            flops=10 * L * L * width,
            bytes_accessed=14 * L * width,
            transcendentals=L * L * head_count,
        ),
    )(queries, key_rows, values, grad, lse, table, column, wide, inverse)


def dp_slice(shard):
    piece = shard.shape[0] // lax.axis_size("dp")
    return lax.dynamic_slice_in_dim(shard, lax.axis_index("dp") * piece, piece, 0)


def gather_in(shard):
    full = lax.all_gather(dp_slice(shard), ("col", "row", "dp"), axis=0, tiled=True)
    return full.reshape(lax.axis_size("col"), D, shard.shape[1])


def gather_out(shard):
    full = lax.all_gather(dp_slice(shard), ("row", "col", "dp"), axis=0, tiled=True)
    return full.reshape(lax.axis_size("row"), -1, shard.shape[1])


def swap(array, axis_name, pairs):
    return lax.ppermute(array, axis_name, pairs)


def add_low(first, second):
    return (first.astype(F32) + second.astype(F32)).astype(BF16)


def take_at(array, index, dim):
    return lax.dynamic_index_in_dim(array, index, dim, keepdims=False)


def flip_pairs(size, mask):
    return [(index, index ^ mask) for index in range(size)]


def ordered(own, other, position, dim):
    first = jnp.where(position == 0, own, other)
    second = jnp.where(position == 0, other, own)
    return jnp.stack((first, second), axis=dim)


def reduce_grad(grad):
    col_size, height, width = grad.shape
    dp_size = lax.axis_size("dp")
    grad = grad.astype(BF16)
    if dp_size != 4 or col_size != 4:
        flat = grad.reshape(col_size * height, width)
        piece = lax.psum_scatter(flat, ("col", "dp"), scatter_dimension=0, tiled=True)
        return lax.all_gather(piece, "dp", axis=0, tiled=True).astype(F32)
    dp_index = lax.axis_index("dp")
    places = (lax.div(dp_index, 2), lax.rem(dp_index, 2))
    masks = (2, 1)
    col_index = lax.axis_index("col")
    high, low = lax.div(col_index, 2), lax.rem(col_index, 2)
    grid = grad.reshape(4, 2, 2, 2, height // 8, width)
    halves = []
    for colour in range(2):
        part = grid[:, :, :, colour]
        first, second = (1, 0) if colour == 0 else (0, 1)
        for axis in (first, second):
            dim = 1 if axis == 0 else part.ndim - 3
            place = places[axis]
            sent = swap(take_at(part, 1 - place, dim), "dp", flip_pairs(4, masks[axis]))
            part = add_low(take_at(part, place, dim), sent)
        halves.append(part)
    both = jnp.stack(halves, axis=1).reshape(2, 2, 2, height // 8, width)
    sent = swap(take_at(both, 1 - low, 1), "col", flip_pairs(4, 1))
    both = add_low(take_at(both, low, 1), sent)
    sent = swap(take_at(both, 1 - high, 0), "col", flip_pairs(4, 2))
    both = add_low(take_at(both, high, 0), sent)
    wholes = []
    for colour in range(2):
        part = both[colour][None, None]
        order = (1, 0) if colour == 0 else (0, 1)
        for axis in order:
            other = swap(part, "dp", flip_pairs(4, masks[axis]))
            joined = ordered(part, other, places[axis], axis)
            shape = list(part.shape)
            shape[axis] = 2
            part = joined.reshape(shape)
        wholes.append(part)
    return jnp.stack(wholes, axis=2).reshape(height, width).astype(F32)


def partner(array):
    return swap(array, "row", [(0, 1), (1, 0)])


def with_partner(array):
    return jnp.concatenate((array, partner(array)), axis=0)


def half_with_partner(array):
    row_index = lax.axis_index("row")
    half = array.shape[1] // 2
    own = lax.dynamic_slice_in_dim(array, row_index * half, half, 1)
    other = lax.dynamic_slice_in_dim(array, (1 - row_index) * half, half, 1)
    return jnp.concatenate((own, partner(other)), axis=0)


def weight_grad_in(rows_low, grads_low, col_size):
    wide = with_partner(grads_low).reshape(2 * grads_low.shape[0], col_size, -1)
    grad = jnp.einsum("td,tcn->cdn", half_with_partner(rows_low), wide, preferred_element_type=F32)
    return reduce_grad(grad.astype(BF16))


def weight_grad_out(hidden_low, grads_low, col_size):
    wide = with_partner(hidden_low)
    grad = jnp.einsum("th,tn->hn", wide, half_with_partner(grads_low), preferred_element_type=F32)
    return reduce_grad(grad.astype(BF16).reshape(col_size, -1, D // 2))


def multiply_in(rows_low, weight):
    return jnp.einsum("td,cdn->tcn", rows_low, weight, preferred_element_type=F32)


def multiply_in_back(grads_low, weight):
    return jnp.einsum("tcn,cdn->td", grads_low, weight, preferred_element_type=F32)


def multiply_out(rows_low, weight):
    return jnp.einsum("th,rhn->trn", rows_low, weight, preferred_element_type=F32).reshape(
        rows_low.shape[0], D
    )


def multiply_out_back(grads_low, weight):
    shaped = grads_low.reshape(grads_low.shape[0], weight.shape[0], -1)
    return jnp.einsum("trn,rhn->th", shaped, weight, preferred_element_type=F32)


def swish_act(values):
    return values * jax.nn.sigmoid(values)


def swish_slope(values):
    sigmoid_rows = jax.nn.sigmoid(values)
    return sigmoid_rows + values * sigmoid_rows * (1.0 - sigmoid_rows)


def norm_forward(stream, gain, shift):
    mean_value = jnp.mean(stream, axis=1, keepdims=True)
    second = jnp.mean(stream * stream, axis=1, keepdims=True)
    inverse = lax.rsqrt(second - mean_value * mean_value + EPSILON)
    return (stream - mean_value) * inverse * gain + shift, (mean_value, inverse)


def norm_backward(grad_rows, gain, stream, saved):
    mean_value, inverse = saved
    normed = (stream - mean_value) * inverse
    scaled = grad_rows * gain
    grad_in = inverse * (
        scaled
        - jnp.mean(scaled, axis=1, keepdims=True)
        - normed * jnp.mean(scaled * normed, axis=1, keepdims=True)
    )
    return grad_in, jnp.sum(grad_rows * normed, axis=0), jnp.sum(grad_rows, axis=0)


def column_sum(rows_low):
    return jnp.sum(rows_low.astype(F32), axis=0)


def ffn_forward(stream, p):
    normed, saved = norm_forward(stream, p["gain"], p["shift"])
    low = normed.astype(BF16)
    hidden_pre = multiply_in(low, p["in"]).reshape(stream.shape[0], -1) + p["bias"]
    hidden = swish_act(hidden_pre).astype(BF16)
    branch = multiply_out(hidden, p["out"])
    return stream + 0.5 * (branch + p["out_bias"]), (stream, saved, low, hidden_pre, hidden)


def ffn_backward(grad, p, kept):
    stream, saved, low, hidden_pre, hidden = kept
    col_size = p["in"].shape[0]
    branch_low = (0.5 * grad).astype(BF16)
    pre_low = (multiply_out_back(branch_low, p["out"]) * swish_slope(hidden_pre)).astype(BF16)
    found = {
        "out": weight_grad_out(hidden, branch_low, col_size),
        "out_bias": column_sum(branch_low),
        "bias": column_sum(pre_low),
        "in": weight_grad_in(low, pre_low, col_size),
    }
    normed_grad = multiply_in_back(pre_low.reshape(pre_low.shape[0], col_size, -1), p["in"])
    input_part, found["gain"], found["shift"] = norm_backward(normed_grad, p["gain"], stream, saved)
    return grad + input_part, found


def halo_pairs(members, forward):
    row_size, col_size = lax.axis_size("row"), lax.axis_size("col")
    pairs = []
    for index in range(row_size * col_size - 1):
        if (index + 1) % members == 0:
            continue
        here = (index % row_size) * col_size + index // row_size
        there = ((index + 1) % row_size) * col_size + (index + 1) // row_size
        pairs.append((here, there) if forward else (there, here))
    return pairs


def local(
    inputs,
    positions,
    grad_output,
    ffn1_norm_gain,
    ffn1_norm_shift,
    ffn1_in,
    ffn1_in_bias,
    ffn1_out,
    ffn1_out_bias,
    attn_norm_gain,
    attn_norm_shift,
    query_weight,
    query_bias,
    key_weight,
    value_weight,
    value_bias,
    distance_table,
    attn_out,
    attn_out_bias,
    conv_norm_gain,
    conv_norm_shift,
    glu_value,
    glu_gate,
    depth_kernel,
    depth_norm_gain,
    depth_norm_shift,
    conv_out,
    ffn2_norm_gain,
    ffn2_norm_shift,
    ffn2_in,
    ffn2_in_bias,
    ffn2_out,
    ffn2_out_bias,
    final_norm_gain,
    final_norm_shift,
):
    row_size, col_size = lax.axis_size("row"), lax.axis_size("col")
    device_count = row_size * col_size
    tokens = inputs.shape[0] // device_count
    members = L // tokens
    me = chunk_index()
    to_float = lambda vector: vector.astype(F32)

    small = jnp.stack(
        (
            ffn1_norm_gain,
            ffn1_norm_shift,
            ffn1_out_bias,
            attn_norm_gain,
            attn_norm_shift,
            attn_out_bias,
            conv_norm_gain,
            conv_norm_shift,
            ffn2_norm_gain,
            ffn2_norm_shift,
            ffn2_out_bias,
            final_norm_gain,
            final_norm_shift,
        )
    )
    small = lax.all_gather(small, ("row", "col"), axis=1, tiled=True).astype(F32)
    first = {
        "gain": small[0],
        "shift": small[1],
        "in": gather_in(ffn1_in),
        "bias": to_float(ffn1_in_bias),
        "out": gather_out(ffn1_out),
        "out_bias": small[2],
    }
    qkv = gather_in(jnp.concatenate((query_weight, key_weight, value_weight), axis=1))
    attn_weight = gather_out(attn_out)
    glu = gather_in(jnp.concatenate((glu_value, glu_gate), axis=1))
    conv_weight = gather_out(conv_out)
    second = {
        "gain": small[8],
        "shift": small[9],
        "in": gather_in(ffn2_in),
        "bias": to_float(ffn2_in_bias),
        "out": gather_out(ffn2_out),
        "out_bias": small[10],
    }

    stream_in, grad_rows = exchange([inputs, grad_output], device_count, True, 0, True)
    stream_in = to_float(stream_in)
    clip_start = lax.div(me, members) * L
    places = lax.dynamic_slice_in_dim(positions, clip_start, L, 0)
    column, wide, inverse = clip_places(places)
    table = jnp.pad(distance_table, ((0, LANES - BUCKETS), (0, 0)))

    stream_one, kept_first = ffn_forward(stream_in, first)

    normed, attn_saved = norm_forward(stream_one, small[3], small[4])
    attn_low = normed.astype(BF16)
    projected = multiply_in(attn_low, qkv).reshape(tokens, col_size, 3, -1)
    own_queries = (projected[:, :, 0].reshape(tokens, D) + to_float(query_bias)).astype(BF16)
    own_keys = projected[:, :, 1].reshape(tokens, D).astype(BF16)
    own_values = (projected[:, :, 2].reshape(tokens, D) + to_float(value_bias)).astype(BF16)
    queries, key_rows, values = exchange([own_queries, own_keys, own_values], members, False, 1)
    mixed, lse = attend(queries, key_rows, values, table, column, wide)
    (own_mixed,) = exchange([mixed], members, True, 2)
    stream_two = stream_one + multiply_out(own_mixed, attn_weight) + small[5]

    normed, conv_saved = norm_forward(stream_two, small[6], small[7])
    conv_low = normed.astype(BF16)
    projected = multiply_in(conv_low, glu).reshape(tokens, col_size, 2, -1)
    glu_rows = projected[:, :, 0].reshape(tokens, D)
    gate_sigmoid = jax.nn.sigmoid(projected[:, :, 1].reshape(tokens, D))
    mixed_rows = glu_rows * gate_sigmoid
    axes = ("row", "col")
    before = lax.ppermute(mixed_rows[tokens - 32 :], axes, halo_pairs(members, True))
    padded = jnp.concatenate((before[2:], mixed_rows), axis=0)
    kernel = to_float(depth_kernel)
    depth_out = kernel[0] * padded[0:tokens]
    for tap in range(1, KERNEL):
        depth_out = depth_out + kernel[tap] * padded[tap : tap + tokens]
    depth_gain, depth_shift = to_float(depth_norm_gain), to_float(depth_norm_shift)
    inner_rows, inner_saved = norm_forward(depth_out, depth_gain, depth_shift)
    act_low = swish_act(inner_rows).astype(BF16)
    stream_three = stream_two + multiply_out(act_low, conv_weight)

    stream_four, kept_second = ffn_forward(stream_three, second)
    final_rows, final_saved = norm_forward(stream_four, small[11], small[12])
    (output,) = exchange([final_rows.astype(BF16)], device_count, False, 3, True)

    grads = {}
    grad_four, final_gain_grad, final_shift_grad = norm_backward(
        to_float(grad_rows), small[11], stream_four, final_saved
    )
    grad_three, second_grads = ffn_backward(grad_four, second, kept_second)

    branch_low = grad_three.astype(BF16)
    conv_out_grad = weight_grad_out(act_low, branch_low, col_size)
    act_grad = multiply_out_back(branch_low, conv_weight)
    depth_grad, depth_gain_grad, depth_shift_grad = norm_backward(
        act_grad * swish_slope(inner_rows), depth_gain, depth_out, inner_saved
    )
    after = lax.ppermute(depth_grad[:32], axes, halo_pairs(members, False))
    padded_grad = jnp.concatenate((depth_grad, after[:30]), axis=0)
    mixed_grad = kernel[0] * padded_grad[KERNEL - 1 : KERNEL - 1 + tokens]
    kernel_rows = [jnp.sum(depth_grad * padded[0:tokens], axis=0)]
    for tap in range(1, KERNEL):
        mixed_grad = (
            mixed_grad + kernel[tap] * padded_grad[KERNEL - 1 - tap : KERNEL - 1 - tap + tokens]
        )
        kernel_rows.append(jnp.sum(depth_grad * padded[tap : tap + tokens], axis=0))
    value_low = (mixed_grad * gate_sigmoid).astype(BF16)
    gate_low = (mixed_grad * glu_rows * gate_sigmoid * (1.0 - gate_sigmoid)).astype(BF16)
    pair_low = jnp.stack(
        (value_low.reshape(tokens, col_size, -1), gate_low.reshape(tokens, col_size, -1)), axis=2
    ).reshape(tokens, col_size, -1)
    glu_grad = weight_grad_in(conv_low, pair_low.reshape(tokens, -1), col_size)
    input_part, conv_gain_grad, conv_shift_grad = norm_backward(
        multiply_in_back(pair_low, glu), small[6], stream_two, conv_saved
    )
    grad_two = grad_three + input_part

    branch_low = grad_two.astype(BF16)
    attn_bias_grad = column_sum(branch_low)
    attn_out_grad = weight_grad_out(own_mixed, branch_low, col_size)
    own_grad = multiply_out_back(branch_low, attn_weight).astype(BF16)
    (mixed_grad,) = exchange([own_grad], members, False, 4)
    query_grad, key_grad, value_grad, table_grad = attend_back(
        queries, key_rows, values, mixed_grad, lse, table, column, wide, inverse
    )
    query_low, key_low, value_low = exchange(
        [query_grad, key_grad, value_grad], members, True, 5
    )
    triple_low = jnp.stack(
        [rows.reshape(tokens, col_size, -1) for rows in (query_low, key_low, value_low)], axis=2
    ).reshape(tokens, col_size, -1)
    qkv_grad = weight_grad_in(attn_low, triple_low.reshape(tokens, -1), col_size)
    input_part, attn_gain_grad, attn_shift_grad = norm_backward(
        multiply_in_back(triple_low, qkv), small[3], stream_one, attn_saved
    )
    grad_one = grad_two + input_part
    grad_zero, first_grads = ffn_backward(grad_one, first, kept_first)
    (input_grad,) = exchange([grad_zero.astype(BF16)], device_count, False, 6, True)

    every = ("dp", "row", "col")
    early = [
        second_grads["bias"],
        jnp.concatenate(kernel_rows),
        depth_gain_grad,
        depth_shift_grad,
        final_gain_grad,
        final_shift_grad,
        second_grads["gain"],
        second_grads["shift"],
        second_grads["out_bias"],
        conv_gain_grad,
        conv_shift_grad,
        attn_bias_grad,
        table_grad[:BUCKETS].reshape(-1),
        column_sum(query_low),
        column_sum(value_low),
        attn_gain_grad,
        attn_shift_grad,
    ]
    late = [
        first_grads["bias"],
        first_grads["out_bias"],
        first_grads["gain"],
        first_grads["shift"],
    ]

    def reduce_small(vectors):
        flat = jnp.concatenate(vectors)
        length = flat.shape[0]
        flat = jnp.pad(flat, (0, -length % LANES)).reshape(-1, LANES)
        flat = lax.psum(flat, every).reshape(-1)
        found = []
        start = 0
        for vector in vectors:
            found.append(flat[start : start + vector.shape[0]])
            start += vector.shape[0]
        return found

    early = reduce_small(early)
    late = reduce_small(late)
    piece = D // device_count
    piece_start = (lax.axis_index("row") * col_size + lax.axis_index("col")) * piece
    own = lambda vector: lax.dynamic_slice_in_dim(vector, piece_start, piece, 0)
    qkv_width = qkv_grad.shape[1] // 3
    glu_width = glu_grad.shape[1] // 2
    return (
        output,
        to_float(input_grad),
        own(late[2]),
        own(late[3]),
        first_grads["in"],
        late[0],
        first_grads["out"],
        own(late[1]),
        own(early[15]),
        own(early[16]),
        qkv_grad[:, :qkv_width],
        early[13],
        qkv_grad[:, qkv_width : 2 * qkv_width],
        qkv_grad[:, 2 * qkv_width :],
        early[14],
        early[12].reshape(BUCKETS, HEAD),
        attn_out_grad,
        own(early[11]),
        own(early[9]),
        own(early[10]),
        glu_grad[:, :glu_width],
        glu_grad[:, glu_width:],
        early[1].reshape(KERNEL, D),
        early[2],
        early[3],
        conv_out_grad,
        own(early[6]),
        own(early[7]),
        second_grads["in"],
        early[0],
        second_grads["out"],
        own(early[8]),
        own(early[4]),
        own(early[5]),
    )


def solution(mesh):
    in_specs = (
        P("dp", ("row", "col")),
        P("dp"),
        P("dp", ("row", "col")),
        P(("row", "col")),
        P(("row", "col")),
        P("row", "col"),
        P(),
        P("col", "row"),
        P(("row", "col")),
        P(("row", "col")),
        P(("row", "col")),
        P("row", "col"),
        P(),
        P("row", "col"),
        P("row", "col"),
        P(),
        P(),
        P("col", "row"),
        P(("row", "col")),
        P(("row", "col")),
        P(("row", "col")),
        P("row", "col"),
        P("row", "col"),
        P(),
        P(),
        P(),
        P("col", "row"),
        P(("row", "col")),
        P(("row", "col")),
        P("row", "col"),
        P(),
        P("col", "row"),
        P(("row", "col")),
        P(("row", "col")),
        P(("row", "col")),
    )
    out_specs = (
        P("dp", ("row", "col")),
        P("dp", ("row", "col")),
        P(("row", "col")),
        P(("row", "col")),
        P("row", "col"),
        P(),
        P("col", "row"),
        P(("row", "col")),
        P(("row", "col")),
        P(("row", "col")),
        P("row", "col"),
        P(),
        P("row", "col"),
        P("row", "col"),
        P(),
        P(),
        P("col", "row"),
        P(("row", "col")),
        P(("row", "col")),
        P(("row", "col")),
        P("row", "col"),
        P("row", "col"),
        P(),
        P(),
        P(),
        P("col", "row"),
        P(("row", "col")),
        P(("row", "col")),
        P("row", "col"),
        P(),
        P("col", "row"),
        P(("row", "col")),
        P(("row", "col")),
        P(("row", "col")),
    )
    return jax.shard_map(local, mesh=mesh, in_specs=in_specs, out_specs=out_specs, check_vma=False)
```

```python
import functools

import jax
import jax.numpy as jnp
from jax import lax
from jax.experimental import pallas as pl
from jax.experimental.pallas import tpu as pltpu
from jax.sharding import PartitionSpec as P

D = 1024
HEAD = 64
FF = 4096
KERNEL = 31
LEFT = 64
RIGHT = 8
L = 1280
BUCKETS = LEFT + RIGHT + 1
EPSILON = 1e-05
SCALE = HEAD ** (-0.5)
LANES = 128
TQ = 256
EDGE = 128
WINDOW = TQ + 2 * EDGE
F32 = jnp.float32
BF16 = jnp.bfloat16
MESH = pl.DeviceIdType.MESH


def chunk_index():
    return lax.axis_index("col") * lax.axis_size("row") + lax.axis_index("row")


def exchange_kernel(count, members, feature_order, to_cols, *refs):
    sources = refs[:count]
    targets = refs[count : 2 * count]
    send_sem, recv_sem, own_sem = refs[2 * count :]
    row_size = lax.axis_size("row")
    col_size = lax.axis_size("col")
    me = lax.axis_index("col") * row_size + lax.axis_index("row")
    member = lax.rem(me, members)
    base = me - member

    def place(index):
        return {"row": lax.rem(index, row_size), "col": lax.div(index, row_size)}

    def column_of(index):
        if feature_order:
            return lax.rem(index, row_size) * col_size + lax.div(index, row_size)
        return lax.rem(index, members)

    def views(number, peer, peer_member):
        source, target = sources[number], targets[number]
        if to_cols:
            rows, width = target.shape[0], source.shape[1]
            return (
                source.at[pl.ds(pl.multiple_of(peer_member * rows, rows), rows), :],
                target.at[:, pl.ds(pl.multiple_of(column_of(me) * width, width), width)],
            )
        rows, width = source.shape[0], target.shape[1]
        return (
            source.at[:, pl.ds(pl.multiple_of(column_of(peer) * width, width), width)],
            target.at[pl.ds(pl.multiple_of(member * rows, rows), rows), :],
        )

    barrier = pltpu.get_barrier_semaphore()
    peers = []
    for step in range(1, members):
        peer_member = lax.rem(member + step, members)
        peers.append((base + peer_member, peer_member))
    for peer, unused in peers:
        pl.semaphore_signal(barrier, inc=1, device_id=place(peer), device_id_type=MESH)
    pl.semaphore_wait(barrier, members - 1)
    copies = []
    for step, (peer, peer_member) in enumerate(peers):
        for number in range(count):
            source, target = views(number, peer, peer_member)
            copy = pltpu.make_async_remote_copy(
                src_ref=source,
                dst_ref=target,
                send_sem=send_sem.at[step * count + number],
                recv_sem=recv_sem.at[step * count + number],
                device_id=place(peer),
                device_id_type=MESH,
            )
            copy.start()
            copies.append(copy)
    for number in range(count):
        source, target = views(number, me, member)
        copy = pltpu.make_async_copy(source, target, own_sem.at[number])
        copy.start()
        copies.append(copy)
    for copy in copies:
        copy.wait()


def narrow_exchange(array, members, to_cols):
    if to_cols:
        rows = array.shape[0] // members
        full = lax.all_gather(array, ("row", "col"), axis=1, tiled=True)
        return lax.dynamic_slice_in_dim(full, chunk_index() * rows, rows, 0)
    width = array.shape[1] // members
    full = lax.all_gather(array, ("col", "row"), axis=0, tiled=True)
    column = lax.axis_index("row") * lax.axis_size("col") + lax.axis_index("col")
    return lax.dynamic_slice_in_dim(full, column * width, width, 1)


def exchange(arrays, members, to_cols, call_id, feature_order=False):
    count = len(arrays)
    if feature_order and D // members < LANES:
        return [narrow_exchange(array, members, to_cols) for array in arrays]
    shapes = []
    for array in arrays:
        height, width = array.shape
        if to_cols:
            shapes.append(jax.ShapeDtypeStruct((height // members, width * members), array.dtype))
        else:
            shapes.append(jax.ShapeDtypeStruct((height * members, width // members), array.dtype))
    any_spec = pl.BlockSpec(memory_space=pl.ANY)
    return pl.pallas_call(
        functools.partial(exchange_kernel, count, members, feature_order, to_cols),
        out_shape=shapes,
        in_specs=[any_spec] * count,
        out_specs=[any_spec] * count,
        scratch_shapes=[
            pltpu.SemaphoreType.DMA(((members - 1) * count,)),
            pltpu.SemaphoreType.DMA(((members - 1) * count,)),
            pltpu.SemaphoreType.DMA((count,)),
        ],
        compiler_params=pltpu.CompilerParams(collective_id=call_id, has_side_effects=True),
    )(*arrays)


def contract(left, right, left_dim, right_dim):
    return lax.dot_general(
        left, right, (((left_dim,), (right_dim,)), ((), ())), preferred_element_type=F32
    )


def head_of(ref, head):
    return ref[:, head * HEAD : (head + 1) * HEAD]


def biased_scores(query, key_rows, table, buckets, row_start, score_ref):
    toward = contract(query, table, 1, 1)
    columns = lax.broadcasted_iota(jnp.int32, (1, L), 1)
    outer = jnp.where(
        columns < row_start - EDGE,
        toward[:, 0:1],
        jnp.where(columns < row_start + TQ + EDGE, 0.0, toward[:, BUCKETS - 1 : BUCKETS]),
    )
    score_ref[:, EDGE : EDGE + L] = contract(query, key_rows, 1, 1) + outer
    for block in range(WINDOW // LANES):
        lanes = pl.ds(pl.multiple_of(row_start + block * LANES, LANES), LANES)
        picked = jnp.take_along_axis(
            toward, buckets[:, block * LANES : (block + 1) * LANES], axis=1
        )
        score_ref[:, lanes] = score_ref[:, lanes] + picked
    return score_ref[:, EDGE : EDGE + L] * SCALE


def window_buckets(place_ref, wide_ref, row_start):
    lanes = pl.ds(pl.multiple_of(row_start, LANES), WINDOW)
    return jnp.clip(wide_ref[:, lanes] - place_ref[...], -LEFT, RIGHT) + LEFT


def attend_kernel(q_ref, k_ref, v_ref, table_ref, place_ref, wide_ref, o_ref, lse_ref, score_ref):
    row_start = pl.program_id(0) * TQ
    buckets = window_buckets(place_ref, wide_ref, row_start)
    table = table_ref[...]
    head_count = q_ref.shape[1] // HEAD
    parts = []
    sums = []
    for head in range(head_count):
        scores = biased_scores(
            head_of(q_ref, head), head_of(k_ref, head), table, buckets, row_start, score_ref
        )
        row_max = jnp.max(scores, axis=1, keepdims=True)
        weights = jnp.exp(scores - row_max)
        total = jnp.sum(weights, axis=1, keepdims=True)
        low = (weights * (1.0 / total)).astype(BF16)
        parts.append(contract(low, head_of(v_ref, head), 1, 0).astype(BF16))
        sums.append(row_max + jnp.log(total))
    o_ref[...] = jnp.concatenate(parts, axis=1)
    lse_ref[...] = jnp.concatenate(sums, axis=1)


def split_low(values):
    high = values.astype(BF16)
    return high, (values - high.astype(F32)).astype(BF16)


def attend_back_kernel(
    q_ref,
    k_ref,
    v_ref,
    go_ref,
    lse_ref,
    table_ref,
    place_ref,
    wide_ref,
    inverse_ref,
    gq_ref,
    gk_ref,
    gv_ref,
    gt_ref,
    score_ref,
    gk_sum,
    gv_sum,
):
    step = pl.program_id(0)
    row_start = step * TQ
    buckets = window_buckets(place_ref, wide_ref, row_start)
    table = table_ref[...]
    inverse = inverse_ref[...] - (row_start - EDGE)
    offsets = wide_ref[:, EDGE : EDGE + L] - place_ref[...]
    low_edge = offsets <= -LEFT
    high_edge = offsets >= RIGHT
    bucket_lane = lax.broadcasted_iota(jnp.int32, (TQ, LANES), 1)
    head_count = q_ref.shape[1] // HEAD

    @pl.when(step == 0)
    def clear():
        gk_sum[...] = jnp.zeros_like(gk_sum)
        gv_sum[...] = jnp.zeros_like(gv_sum)
        gt_ref[...] = jnp.zeros_like(gt_ref)

    gq_parts = []
    gk_parts = []
    gv_parts = []
    table_grad = jnp.zeros((LANES, HEAD), F32)
    for head in range(head_count):
        query = head_of(q_ref, head)
        key_rows = head_of(k_ref, head)
        grad = head_of(go_ref, head)
        scores = biased_scores(query, key_rows, table, buckets, row_start, score_ref)
        probs = jnp.exp(scores - lse_ref[:, head : head + 1])
        prob_grad = contract(grad, head_of(v_ref, head), 1, 1)
        inner = jnp.sum(probs * prob_grad, axis=1, keepdims=True)
        score_grad = (probs * (prob_grad - inner)).astype(BF16)
        gv_parts.append(contract(probs.astype(BF16), grad, 0, 0))
        gk_parts.append(contract(score_grad, query, 0, 0) * SCALE)
        wide_grad = score_grad.astype(F32)
        low_total = jnp.sum(jnp.where(low_edge, wide_grad, 0.0), axis=1, keepdims=True)
        high_total = jnp.sum(jnp.where(high_edge, wide_grad, 0.0), axis=1, keepdims=True)
        score_ref[:, EDGE : EDGE + L] = wide_grad
        spread = jnp.where(
            bucket_lane == 0, low_total, jnp.where(bucket_lane == BUCKETS - 1, high_total, 0.0)
        )
        for block in range(WINDOW // LANES):
            lanes = pl.ds(pl.multiple_of(row_start + block * LANES, LANES), LANES)
            local = inverse - block * LANES
            inside = (local >= 0) & (local < LANES)
            picked = jnp.take_along_axis(
                score_ref[:, lanes], jnp.clip(local, 0, LANES - 1), axis=1
            )
            spread = spread + jnp.where(inside, picked, 0.0)
        spread_high, spread_low = split_low(spread)
        gq_parts.append(
            (
                (
                    contract(score_grad, key_rows, 1, 0)
                    + (contract(spread_high, table, 1, 0) + contract(spread_low, table, 1, 0))
                )
                * SCALE
            ).astype(BF16)
        )
        table_grad = table_grad + (
            contract(spread_high, query, 0, 0) + contract(spread_low, query, 0, 0)
        )
    gq_ref[...] = jnp.concatenate(gq_parts, axis=1)
    gk_sum[...] += jnp.concatenate(gk_parts, axis=1)
    gv_sum[...] += jnp.concatenate(gv_parts, axis=1)
    gt_ref[...] += table_grad * SCALE

    @pl.when(step == pl.num_programs(0) - 1)
    def flush():
        gk_ref[...] = gk_sum[...].astype(BF16)
        gv_ref[...] = gv_sum[...].astype(BF16)


def inverse_kernel(place_ref, band_ref, inverse_ref):
    row_start = pl.program_id(0) * TQ
    lane = lax.broadcasted_iota(jnp.int32, (TQ, LANES), 1)
    valid = (lane > 0) & (lane < BUCKETS - 1)
    target = place_ref[...] + (lane - LEFT)
    found = jnp.full((TQ, LANES), -(1 << 20), jnp.int32)
    for shift in range(1 - LEFT, RIGHT):
        column = band_ref[pl.ds(row_start + EDGE + shift, TQ), :]
        found = jnp.where(column == target, shift, found)
    key_index = found + lax.broadcasted_iota(jnp.int32, (TQ, LANES), 0) + row_start
    inverse_ref[...] = jnp.where(valid, key_index, -(1 << 20))


def clip_places(places):
    column = places[:, None]
    wide = jnp.pad(places, (EDGE, EDGE))
    band = jnp.pad(places, (EDGE, EDGE), constant_values=-(1 << 20))
    band = jnp.broadcast_to(band[:, None], (L + 2 * EDGE, LANES))
    inverse = pl.pallas_call(
        inverse_kernel,
        grid=(L // TQ,),
        out_shape=jax.ShapeDtypeStruct((L, LANES), jnp.int32),
        in_specs=[
            pl.BlockSpec((TQ, 1), lambda i: (i, 0)),
            pl.BlockSpec((L + 2 * EDGE, LANES), lambda i: (0, 0)),
        ],
        out_specs=pl.BlockSpec((TQ, LANES), lambda i: (i, 0)),
    )(column, band)
    return column, wide[None, :], inverse


def attend(queries, key_rows, values, table, column, wide):
    width = queries.shape[1]
    head_count = width // HEAD
    tile = pl.BlockSpec((TQ, width), lambda i: (i, 0))
    whole = pl.BlockSpec((L, width), lambda i: (0, 0))
    return pl.pallas_call(
        attend_kernel,
        grid=(L // TQ,),
        out_shape=[
            jax.ShapeDtypeStruct((L, width), BF16),
            jax.ShapeDtypeStruct((L, head_count), F32),
        ],
        in_specs=[
            tile,
            whole,
            whole,
            pl.BlockSpec((LANES, HEAD), lambda i: (0, 0)),
            pl.BlockSpec((TQ, 1), lambda i: (i, 0)),
            pl.BlockSpec((1, L + 2 * EDGE), lambda i: (0, 0)),
        ],
        out_specs=[tile, pl.BlockSpec((TQ, head_count), lambda i: (i, 0))],
        scratch_shapes=[pltpu.VMEM((TQ, L + 2 * EDGE), F32)],
        cost_estimate=pl.CostEstimate(
            flops=4 * L * L * width, bytes_accessed=8 * L * width, transcendentals=L * L * head_count
        ),
    )(queries, key_rows, values, table, column, wide)


def attend_back(queries, key_rows, values, grad, lse, table, column, wide, inverse):
    width = queries.shape[1]
    head_count = width // HEAD
    tile = pl.BlockSpec((TQ, width), lambda i: (i, 0))
    whole = pl.BlockSpec((L, width), lambda i: (0, 0))
    return pl.pallas_call(
        attend_back_kernel,
        grid=(L // TQ,),
        out_shape=[
            jax.ShapeDtypeStruct((L, width), BF16),
            jax.ShapeDtypeStruct((L, width), BF16),
            jax.ShapeDtypeStruct((L, width), BF16),
            jax.ShapeDtypeStruct((LANES, HEAD), F32),
        ],
        in_specs=[
            tile,
            whole,
            whole,
            tile,
            pl.BlockSpec((TQ, head_count), lambda i: (i, 0)),
            pl.BlockSpec((LANES, HEAD), lambda i: (0, 0)),
            pl.BlockSpec((TQ, 1), lambda i: (i, 0)),
            pl.BlockSpec((1, L + 2 * EDGE), lambda i: (0, 0)),
            pl.BlockSpec((TQ, LANES), lambda i: (i, 0)),
        ],
        out_specs=[tile, whole, whole, pl.BlockSpec((LANES, HEAD), lambda i: (0, 0))],
        scratch_shapes=[
            pltpu.VMEM((TQ, L + 2 * EDGE), F32),
            pltpu.VMEM((L, width), F32),
            pltpu.VMEM((L, width), F32),
        ],
        cost_estimate=pl.CostEstimate(
            flops=10 * L * L * width,
            bytes_accessed=14 * L * width,
            transcendentals=L * L * head_count,
        ),
    )(queries, key_rows, values, grad, lse, table, column, wide, inverse)


def dp_slice(shard):
    piece = shard.shape[0] // lax.axis_size("dp")
    return lax.dynamic_slice_in_dim(shard, lax.axis_index("dp") * piece, piece, 0)


def gather_in(shard):
    full = lax.all_gather(dp_slice(shard), ("col", "row", "dp"), axis=0, tiled=True)
    return full.reshape(lax.axis_size("col"), D, shard.shape[1])


def gather_out(shard):
    full = lax.all_gather(dp_slice(shard), ("row", "col", "dp"), axis=0, tiled=True)
    return full.reshape(lax.axis_size("row"), -1, shard.shape[1])


def regular_grid():
    return lax.axis_size("dp") == 4 and lax.axis_size("col") == 4 and lax.axis_size("row") == 2


def split_lanes(array, width):
    return [array[:, start : start + width] for start in range(0, array.shape[1], width)]


def gather_weights(in_shards, out_shards):
    if not regular_grid():
        return [InWeight(gather_in(jnp.concatenate(group, axis=1))) for group in in_shards] + [
            OutWeight(gather_out(shard)) for shard in out_shards
        ]
    width = D // lax.axis_size("col")
    pieces = []
    handles = []
    height = 0
    for group in in_shards:
        count = 0
        rows = 0
        for shard in group:
            piece = dp_slice(shard)
            rows = piece.shape[0]
            lanes = split_lanes(piece, width)
            pieces += lanes
            count += len(lanes)
        handles.append((InWeight, height // rows, count, rows))
        height += count * rows
    for shard in out_shards:
        piece = dp_slice(shard)
        rows = piece.shape[0]
        lanes = split_lanes(piece, width)
        if height % rows:
            pieces.append(jnp.zeros((-height % rows, width), piece.dtype))
            height += -height % rows
        pieces += lanes
        handles.append((OutWeight, height // rows, len(lanes), rows))
        height += len(lanes) * rows
    full = lax.all_gather(jnp.concatenate(pieces, axis=0), ("col", "row", "dp"), axis=0)
    full = full.reshape(4, 2, 4, height, width)
    return [kind(full, block, count, rows) for kind, block, count, rows in handles]


def in_kernel(count, joined, rows_ref, *refs):
    rows = rows_ref[...]
    width = refs[0].shape[-1]
    for number in range(count):
        product = jnp.dot(rows, refs[number][...].reshape(D, width), preferred_element_type=F32)
        if joined:
            refs[count][:, number * width : (number + 1) * width] = product
        else:
            refs[count + number][...] = product


def in_back_kernel(count, grads_ref, *refs):
    target = refs[count]
    width = refs[0].shape[-1]
    total = None
    for number in range(count):
        term = contract(
            grads_ref[:, number * width : (number + 1) * width],
            refs[number][...].reshape(D, width),
            1,
            1,
        )
        total = term if total is None else total + term

    @pl.when(pl.program_id(0) == 0)
    def first():
        target[...] = total

    @pl.when(pl.program_id(0) > 0)
    def later():
        target[...] += total


def out_kernel(rows_ref, weight_ref, target):
    width = weight_ref.shape[-1]
    weight = weight_ref[...].reshape(rows_ref.shape[1], width)
    target[...] = jnp.dot(rows_ref[...], weight, preferred_element_type=F32)


def out_back_kernel(count, grads_ref, *refs):
    target = refs[count]
    width = refs[0].shape[-1]
    height = target.shape[1]
    total = None
    for half in range(2):
        for number in range(count):
            start = (half * count + number) * width
            term = contract(
                grads_ref[:, start : start + width],
                refs[number][0, half].reshape(height, width),
                1,
                1,
            )
            total = term if total is None else total + term
    target[...] = total


def matmul_cost(tokens, wide, outer):
    return pl.CostEstimate(
        flops=2 * tokens * D * wide,
        bytes_accessed=2 * D * wide + 4 * tokens * outer + 2 * tokens * (D + wide - outer),
        transcendentals=0,
    )


class InWeight:
    def __init__(self, full, block=None, count=None, rows=None):
        self.full, self.block, self.count, self.rows = full, block, count, rows

    def specs(self):
        width = self.full.shape[-1]
        return [
            pl.BlockSpec(
                (1, 2, 4, self.rows, width), lambda c, at=self.block + number: (c, 0, 0, at, 0)
            )
            for number in range(self.count)
        ]

    def forward(self, rows_low, parts):
        tokens = rows_low.shape[0]
        if self.block is None:
            product = jnp.einsum("td,cdn->tcn", rows_low, self.full, preferred_element_type=F32)
            if parts == 1:
                return product.reshape(tokens, -1)
            product = product.reshape(tokens, product.shape[1], parts, -1)
            return [product[:, :, part].reshape(tokens, D) for part in range(parts)]
        width = self.full.shape[-1]
        joined = parts == 1
        wide = 4 * self.count * width
        if joined:
            shapes = jax.ShapeDtypeStruct((tokens, wide), F32)
            out_specs = pl.BlockSpec((tokens, self.count * width), lambda c: (0, c))
        else:
            shapes = [jax.ShapeDtypeStruct((tokens, D), F32)] * parts
            out_specs = [pl.BlockSpec((tokens, width), lambda c: (0, c))] * parts
        return pl.pallas_call(
            functools.partial(in_kernel, self.count, joined),
            grid=(4,),
            out_shape=shapes,
            in_specs=[pl.BlockSpec((tokens, D), lambda c: (0, 0))] + self.specs(),
            out_specs=out_specs,
            cost_estimate=matmul_cost(tokens, wide, wide),
        )(rows_low, *([self.full] * self.count))

    def backward(self, grads_low):
        tokens, wide = grads_low.shape
        if self.block is None:
            shaped = grads_low.reshape(tokens, self.full.shape[0], -1)
            return jnp.einsum("tcn,cdn->td", shaped, self.full, preferred_element_type=F32)
        return pl.pallas_call(
            functools.partial(in_back_kernel, self.count),
            grid=(4,),
            out_shape=jax.ShapeDtypeStruct((tokens, D), F32),
            in_specs=[pl.BlockSpec((tokens, wide // 4), lambda c: (0, c))] + self.specs(),
            out_specs=pl.BlockSpec((tokens, D), lambda c: (0, 0)),
            cost_estimate=matmul_cost(tokens, wide, D),
        )(grads_low, *([self.full] * self.count))


class OutWeight:
    def __init__(self, full, block=None, count=None, rows=None):
        self.full, self.block, self.count, self.rows = full, block, count, rows

    def forward(self, rows_low):
        tokens, height = rows_low.shape
        if self.block is None:
            product = jnp.einsum("th,rhn->trn", rows_low, self.full, preferred_element_type=F32)
            return product.reshape(tokens, D)
        width = self.full.shape[-1]
        count, block = self.count, self.block
        return pl.pallas_call(
            out_kernel,
            grid=(2, count),
            out_shape=jax.ShapeDtypeStruct((tokens, D), F32),
            in_specs=[
                pl.BlockSpec((tokens, height), lambda r, n: (0, 0)),
                pl.BlockSpec((4, 1, 4, self.rows, width), lambda r, n: (0, r, 0, block + n, 0)),
            ],
            out_specs=pl.BlockSpec((tokens, width), lambda r, n: (0, r * count + n)),
            cost_estimate=matmul_cost(tokens, height, D),
        )(rows_low, self.full)

    def backward(self, grads_low):
        tokens = grads_low.shape[0]
        if self.block is None:
            shaped = grads_low.reshape(tokens, self.full.shape[0], -1)
            return jnp.einsum("trn,rhn->th", shaped, self.full, preferred_element_type=F32)
        width = self.full.shape[-1]
        height = 4 * self.rows
        specs = [
            pl.BlockSpec(
                (1, 2, 4, self.rows, width), lambda c, at=self.block + number: (c, 0, 0, at, 0)
            )
            for number in range(self.count)
        ]
        return pl.pallas_call(
            functools.partial(out_back_kernel, self.count),
            grid=(4,),
            out_shape=jax.ShapeDtypeStruct((tokens, 4 * height), F32),
            in_specs=[pl.BlockSpec((tokens, D), lambda c: (0, 0))] + specs,
            out_specs=pl.BlockSpec((tokens, height), lambda c: (0, c)),
            cost_estimate=matmul_cost(tokens, 4 * height, 4 * height),
        )(grads_low, *([self.full] * self.count))


def interleave(parts, col_size):
    width = D // col_size
    return jnp.concatenate(
        [part[:, c * width : (c + 1) * width] for c in range(col_size) for part in parts], axis=1
    )


def swap(array, axis_name, pairs):
    return lax.ppermute(array, axis_name, pairs)


def add_low(first, second):
    return (first.astype(F32) + second.astype(F32)).astype(BF16)


def take_at(array, index, dim):
    return lax.dynamic_index_in_dim(array, index, dim, keepdims=False)


def flip_pairs(size, mask):
    return [(index, index ^ mask) for index in range(size)]


def ordered(own, other, position, dim):
    first = jnp.where(position == 0, own, other)
    second = jnp.where(position == 0, other, own)
    return jnp.stack((first, second), axis=dim)


def reduce_steps(grad):
    if not regular_grid():
        flat = grad.reshape(-1, grad.shape[2])
        piece = lax.psum_scatter(flat, ("col", "dp"), scatter_dimension=0, tiled=True)
        return lax.all_gather(piece, "dp", axis=0, tiled=True).astype(F32)
    outer, height, width = grad.shape
    dp_index = lax.axis_index("dp")
    places = (lax.div(dp_index, 2), lax.rem(dp_index, 2))
    masks = (2, 1)
    orders = ((1, 0), (0, 1))
    col_index = lax.axis_index("col")
    grid = grad.reshape(outer, 2, 2, 2, height // 8, width)
    parts = [grid[:, :, :, 0], grid[:, :, :, 1]]
    for step in range(2):
        kept = []
        sent = []
        for part, order in zip(parts, orders):
            axis = order[step]
            dim = 1 if axis == 0 else part.ndim - 3
            kept.append(take_at(part, places[axis], dim))
            sent.append(
                swap(take_at(part, 1 - places[axis], dim), "dp", flip_pairs(4, masks[axis]))
            )
        sent = yield sent
        parts = [add_low(own, other) for own, other in zip(kept, sent)]
    both = jnp.stack(parts, axis=1)
    high, low = lax.div(col_index, 2), lax.rem(col_index, 2)
    both = both.reshape(2, 2, 2, height // 8, width)
    for mask, dim, place in ((1, 1, low), (2, 0, high)):
        kept = take_at(both, place, dim)
        (sent,) = yield [swap(take_at(both, 1 - place, dim), "col", flip_pairs(4, mask))]
        both = add_low(kept, sent)
    wholes = [both[0][None, None], both[1][None, None]]
    for step in range(2):
        sent = yield [
            swap(part, "dp", flip_pairs(4, masks[order[step]]))
            for part, order in zip(wholes, orders)
        ]
        joined = []
        for part, other, order in zip(wholes, sent, orders):
            axis = order[step]
            shape = list(part.shape)
            shape[axis] = 2
            joined.append(ordered(part, other, places[axis], axis).reshape(shape))
        wholes = joined
    return jnp.stack(wholes, axis=2).reshape(height, width).astype(F32)


def total_steps(vectors):
    flat = jnp.concatenate([vector.reshape(-1, D) for vector in vectors], axis=0)
    if not regular_grid():
        flat = lax.psum(flat, ("dp", "row", "col"))
    else:
        for axis_name, size, mask in (
            ("row", 2, 1),
            ("dp", 4, 1),
            ("dp", 4, 2),
            ("col", 4, 1),
            ("col", 4, 2),
        ):
            (other,) = yield [swap(flat, axis_name, flip_pairs(size, mask))]
            flat = flat + other
    found = []
    start = 0
    for vector in vectors:
        rows = vector.size // D
        found.append(flat[start : start + rows].reshape(-1))
        start += rows
    return found


class Pipeline:
    def __init__(self):
        self.active = []
        self.results = {}

    def advance(self, name, steps, arrays):
        try:
            flight = next(steps) if arrays is None else steps.send(arrays)
            self.active.append((name, steps, flight))
        except StopIteration as stop:
            self.results[name] = stop.value

    def start(self, name, steps):
        self.advance(name, steps, None)

    def tie(self, *streams):
        flights = [flight for unused, unused, flight in self.active]
        streams, flights = lax.optimization_barrier((streams, flights))
        current, self.active = self.active, []
        for (name, steps, unused), flight in zip(current, flights):
            self.advance(name, steps, flight)
        return streams[0] if len(streams) == 1 else streams

    def finish(self):
        while self.active:
            self.tie()
        return self.results


def partner(array):
    return swap(array, "row", [(0, 1), (1, 0)])


def with_partner(array):
    return array, partner(array)


def half_with_partner(array):
    row_index = lax.axis_index("row")
    half = array.shape[1] // 2
    own = lax.dynamic_slice_in_dim(array, row_index * half, half, 1)
    other = lax.dynamic_slice_in_dim(array, (1 - row_index) * half, half, 1)
    return own, partner(other)


def weight_grad_kernel(own_rows, other_rows, own_grads, other_grads, target):
    target[0] = (
        contract(own_rows[...], own_grads[...], 0, 0)
        + contract(other_rows[...], other_grads[...], 0, 0)
    ).astype(BF16)


def weight_grad(rows, grads, split_rows, col_size):
    tokens = rows[0].shape[0]
    height, width = rows[0].shape[1], grads[0].shape[1]
    whole = lambda size: pl.BlockSpec((tokens, size), lambda c: (0, 0))
    block = lambda size: pl.BlockSpec((tokens, size), lambda c: (0, c))
    if split_rows:
        height //= col_size
        row_spec, grad_spec = block(height), whole(width)
    else:
        width //= col_size
        row_spec, grad_spec = whole(height), block(width)
    return pl.pallas_call(
        weight_grad_kernel,
        grid=(col_size,),
        out_shape=jax.ShapeDtypeStruct((col_size, height, width), BF16),
        in_specs=[row_spec, row_spec, grad_spec, grad_spec],
        out_specs=pl.BlockSpec((1, height, width), lambda c: (c, 0, 0)),
        cost_estimate=pl.CostEstimate(
            flops=4 * tokens * height * width * col_size,
            bytes_accessed=2 * (2 * tokens * (height + width) + height * width) * col_size,
            transcendentals=0,
        ),
    )(*rows, *grads)


def weight_grad_in(rows_low, grads_low, col_size):
    return weight_grad(half_with_partner(rows_low), with_partner(grads_low), False, col_size)


def weight_grad_out(hidden_low, grads_low, col_size):
    return weight_grad(with_partner(hidden_low), half_with_partner(grads_low), True, col_size)


def scatter_grad(grad):
    flat = grad.reshape(-1, grad.shape[2])
    return lax.psum_scatter(flat, ("col", "dp"), scatter_dimension=0, tiled=True)


def stack_pieces(pieces):
    width = min(piece.shape[1] for piece in pieces)
    return jnp.concatenate([lanes for piece in pieces for lanes in split_lanes(piece, width)], axis=0)


def unstack_pieces(full, shapes):
    width = full.shape[2]
    found = []
    start = 0
    for height, whole in shapes:
        lanes = []
        for unused in range(whole // width):
            lanes.append(full[:, start : start + height].reshape(-1, width))
            start += height
        found.append(jnp.concatenate(lanes, axis=1).astype(F32))
    return found


def swish_act(values):
    return values * jax.nn.sigmoid(values)


def swish_slope(values):
    sigmoid_rows = jax.nn.sigmoid(values)
    return sigmoid_rows + values * sigmoid_rows * (1.0 - sigmoid_rows)


def norm_forward(stream, gain, shift):
    mean_value = jnp.mean(stream, axis=1, keepdims=True)
    second = jnp.mean(stream * stream, axis=1, keepdims=True)
    inverse = lax.rsqrt(second - mean_value * mean_value + EPSILON)
    return (stream - mean_value) * inverse * gain + shift, (mean_value, inverse)


def norm_backward(grad_rows, gain, stream, saved):
    mean_value, inverse = saved
    normed = (stream - mean_value) * inverse
    scaled = grad_rows * gain
    grad_in = inverse * (
        scaled
        - jnp.mean(scaled, axis=1, keepdims=True)
        - normed * jnp.mean(scaled * normed, axis=1, keepdims=True)
    )
    return grad_in, jnp.sum(grad_rows * normed, axis=0), jnp.sum(grad_rows, axis=0)


def column_sum(rows_low):
    return jnp.sum(rows_low.astype(F32), axis=0)


def ffn_forward(stream, p):
    normed, saved = norm_forward(stream, p["gain"], p["shift"])
    low = normed.astype(BF16)
    hidden_pre = p["in"].forward(low, 1) + p["bias"]
    hidden = swish_act(hidden_pre).astype(BF16)
    branch = p["out"].forward(hidden)
    return stream + 0.5 * (branch + p["out_bias"]), (stream, saved, low, hidden_pre, hidden)


def ffn_backward(grad, p, kept, pipe, name, pieces, permuted):
    stream, saved, low, hidden_pre, hidden = kept
    col_size = lax.axis_size("col")
    branch_low = (0.5 * grad).astype(BF16)
    out_grad = weight_grad_out(hidden, branch_low, col_size)
    if permuted:
        pipe.start(name + "_out", reduce_steps(out_grad))
    else:
        branch_low, out_grad = lax.optimization_barrier((branch_low, out_grad))
        pieces[name + "_out"] = scatter_grad(out_grad)
    pre_low = (p["out"].backward(branch_low) * swish_slope(hidden_pre)).astype(BF16)
    found = {"out_bias": column_sum(branch_low), "bias": column_sum(pre_low)}
    if permuted:
        names = list(pieces)
        shapes = [pieces[piece_name].shape for piece_name in names]
        stacked = stack_pieces([pieces[piece_name] for piece_name in names])
        pre_low, in_grad, stacked = pipe.tie(
            pre_low, weight_grad_in(low, pre_low, col_size), stacked
        )
        pipe.start(name + "_in", reduce_steps(in_grad))
        full = lax.all_gather(stacked, "dp", axis=0)
        found["gathered"] = (names, shapes, full)
    else:
        pre_low, in_grad = pipe.tie(pre_low, weight_grad_in(low, pre_low, col_size))
        pieces[name + "_in"] = scatter_grad(in_grad)
    normed_grad = p["in"].backward(pre_low)
    input_part, found["gain"], found["shift"] = norm_backward(normed_grad, p["gain"], stream, saved)
    return grad + input_part, found


def halo_pairs(members, forward):
    row_size, col_size = lax.axis_size("row"), lax.axis_size("col")
    pairs = []
    for index in range(row_size * col_size - 1):
        if (index + 1) % members == 0:
            continue
        here = (index % row_size) * col_size + index // row_size
        there = ((index + 1) % row_size) * col_size + (index + 1) // row_size
        pairs.append((here, there) if forward else (there, here))
    return pairs


def local(
    inputs,
    positions,
    grad_output,
    ffn1_norm_gain,
    ffn1_norm_shift,
    ffn1_in,
    ffn1_in_bias,
    ffn1_out,
    ffn1_out_bias,
    attn_norm_gain,
    attn_norm_shift,
    query_weight,
    query_bias,
    key_weight,
    value_weight,
    value_bias,
    distance_table,
    attn_out,
    attn_out_bias,
    conv_norm_gain,
    conv_norm_shift,
    glu_value,
    glu_gate,
    depth_kernel,
    depth_norm_gain,
    depth_norm_shift,
    conv_out,
    ffn2_norm_gain,
    ffn2_norm_shift,
    ffn2_in,
    ffn2_in_bias,
    ffn2_out,
    ffn2_out_bias,
    final_norm_gain,
    final_norm_shift,
):
    row_size, col_size = lax.axis_size("row"), lax.axis_size("col")
    device_count = row_size * col_size
    tokens = inputs.shape[0] // device_count
    members = L // tokens
    me = chunk_index()
    to_float = lambda vector: vector.astype(F32)

    small = jnp.stack(
        (
            ffn1_norm_gain,
            ffn1_norm_shift,
            ffn1_out_bias,
            attn_norm_gain,
            attn_norm_shift,
            attn_out_bias,
            conv_norm_gain,
            conv_norm_shift,
            ffn2_norm_gain,
            ffn2_norm_shift,
            ffn2_out_bias,
            final_norm_gain,
            final_norm_shift,
        )
    )
    small = jnp.pad(small, ((0, 16 - small.shape[0]), (0, 0)))
    stream_in, grad_rows, small = exchange(
        [inputs, grad_output, jnp.tile(small, (device_count, 1))], device_count, True, 0, True
    )
    small = small.astype(F32)
    first_in, qkv, glu, first_out, attn_weight, conv_weight = gather_weights(
        [[ffn1_in], [query_weight, key_weight, value_weight], [glu_value, glu_gate]],
        [ffn1_out, attn_out, conv_out],
    )
    second_in, second_out = gather_weights([[ffn2_in]], [ffn2_out])
    first = {
        "gain": small[0],
        "shift": small[1],
        "in": first_in,
        "bias": to_float(ffn1_in_bias),
        "out": first_out,
        "out_bias": small[2],
    }
    second = {
        "gain": small[8],
        "shift": small[9],
        "in": second_in,
        "bias": to_float(ffn2_in_bias),
        "out": second_out,
        "out_bias": small[10],
    }

    clip_start = lax.div(me, members) * L
    places = lax.dynamic_slice_in_dim(positions, clip_start, L, 0)
    column, wide, inverse = clip_places(places)
    table = jnp.pad(distance_table, ((0, LANES - BUCKETS), (0, 0)))
    stream_in, inverse = lax.optimization_barrier((stream_in, inverse))
    stream_in = to_float(stream_in)

    stream_one, kept_first = ffn_forward(stream_in, first)

    normed, attn_saved = norm_forward(stream_one, small[3], small[4])
    attn_low = normed.astype(BF16)
    own_queries, own_keys, own_values = qkv.forward(attn_low, 3)
    own_queries = (own_queries + to_float(query_bias)).astype(BF16)
    own_keys = own_keys.astype(BF16)
    own_values = (own_values + to_float(value_bias)).astype(BF16)
    queries, key_rows, values = exchange([own_queries, own_keys, own_values], members, False, 1)
    mixed, lse = attend(queries, key_rows, values, table, column, wide)
    (own_mixed,) = exchange([mixed], members, True, 2)
    stream_two = stream_one + attn_weight.forward(own_mixed) + small[5]

    normed, conv_saved = norm_forward(stream_two, small[6], small[7])
    conv_low = normed.astype(BF16)
    glu_rows, gate_rows = glu.forward(conv_low, 2)
    gate_sigmoid = jax.nn.sigmoid(gate_rows)
    mixed_rows = glu_rows * gate_sigmoid
    axes = ("row", "col")
    before = lax.ppermute(mixed_rows[tokens - 32 :], axes, halo_pairs(members, True))
    padded = jnp.concatenate((before[2:], mixed_rows), axis=0)
    kernel = to_float(depth_kernel)
    depth_out = kernel[0] * padded[0:tokens]
    for tap in range(1, KERNEL):
        depth_out = depth_out + kernel[tap] * padded[tap : tap + tokens]
    depth_gain, depth_shift = to_float(depth_norm_gain), to_float(depth_norm_shift)
    inner_rows, inner_saved = norm_forward(depth_out, depth_gain, depth_shift)
    act_low = swish_act(inner_rows).astype(BF16)
    stream_three = stream_two + conv_weight.forward(act_low)

    stream_four, kept_second = ffn_forward(stream_three, second)
    final_rows, final_saved = norm_forward(stream_four, small[11], small[12])
    (output,) = exchange([final_rows.astype(BF16)], device_count, False, 3, True)

    output, grad_rows = lax.optimization_barrier((output, grad_rows))
    grad_four, final_gain_grad, final_shift_grad = norm_backward(
        to_float(grad_rows), small[11], stream_four, final_saved
    )
    pipe = Pipeline()
    pieces = {}
    grad_three, second_grads = ffn_backward(grad_four, second, kept_second, pipe, "ffn2", pieces, False)

    branch_low = grad_three.astype(BF16)
    conv_out_grad = weight_grad_out(act_low, branch_low, col_size)
    act_grad = conv_weight.backward(branch_low)
    depth_grad, depth_gain_grad, depth_shift_grad = norm_backward(
        act_grad * swish_slope(inner_rows), depth_gain, depth_out, inner_saved
    )
    after = lax.ppermute(depth_grad[:32], axes, halo_pairs(members, False))
    padded_grad = jnp.concatenate((depth_grad, after[:30]), axis=0)
    mixed_grad = kernel[0] * padded_grad[KERNEL - 1 : KERNEL - 1 + tokens]
    kernel_rows = [jnp.sum(depth_grad * padded[0:tokens], axis=0)]
    for tap in range(1, KERNEL):
        mixed_grad = (
            mixed_grad + kernel[tap] * padded_grad[KERNEL - 1 - tap : KERNEL - 1 - tap + tokens]
        )
        kernel_rows.append(jnp.sum(depth_grad * padded[tap : tap + tokens], axis=0))
    value_low = (mixed_grad * gate_sigmoid).astype(BF16)
    gate_low = (mixed_grad * glu_rows * gate_sigmoid * (1.0 - gate_sigmoid)).astype(BF16)
    pair_low = interleave((value_low, gate_low), col_size)
    glu_grad = weight_grad_in(conv_low, pair_low, col_size)
    input_part, conv_gain_grad, conv_shift_grad = norm_backward(
        glu.backward(pair_low), small[6], stream_two, conv_saved
    )
    grad_two = grad_three + input_part

    branch_low = grad_two.astype(BF16)
    attn_bias_grad = column_sum(branch_low)
    attn_out_grad = weight_grad_out(own_mixed, branch_low, col_size)
    own_grad = attn_weight.backward(branch_low).astype(BF16)
    glu_height, out_height = glu_grad.shape[1], conv_out_grad.shape[1]
    out_width = conv_out_grad.shape[2]
    rest = {"outs": jnp.concatenate((attn_out_grad, conv_out_grad), axis=1), "glu": glu_grad}
    if glu_grad.shape[2] == out_width:
        rest = {"rest": jnp.concatenate((glu_grad, rest["outs"]), axis=1)}
    own_grad, rest = pipe.tie(own_grad, rest)
    for piece_name, grad in rest.items():
        pieces[piece_name] = scatter_grad(grad)
    (mixed_grad,) = exchange([own_grad], members, False, 4)
    query_grad, key_grad, value_grad, table_grad = attend_back(
        queries, key_rows, values, mixed_grad, lse, table, column, wide, inverse
    )
    query_grad = pipe.tie(query_grad)
    query_low, key_low, value_low = exchange(
        [query_grad, key_grad, value_grad], members, True, 5
    )
    query_low, key_low, value_low = pipe.tie(query_low, key_low, value_low)
    triple_low = interleave((query_low, key_low, value_low), col_size)
    qkv_grad = weight_grad_in(attn_low, triple_low, col_size)
    input_part, attn_gain_grad, attn_shift_grad = norm_backward(
        qkv.backward(triple_low), small[3], stream_one, attn_saved
    )
    grad_one = grad_two + input_part
    grad_one, qkv_grad = pipe.tie(grad_one, qkv_grad)
    pipe.start("qkv", reduce_steps(qkv_grad))
    early = [
        second_grads["bias"],
        jnp.stack(kernel_rows),
        depth_gain_grad,
        depth_shift_grad,
        final_gain_grad,
        final_shift_grad,
        second_grads["gain"],
        second_grads["shift"],
        second_grads["out_bias"],
        conv_gain_grad,
        conv_shift_grad,
        attn_bias_grad,
        jnp.pad(table_grad[:BUCKETS], ((0, -BUCKETS % 16), (0, 0))),
        column_sum(query_low),
        column_sum(value_low),
        attn_gain_grad,
        attn_shift_grad,
    ]
    pipe.start("early", total_steps(early))
    grad_zero, first_grads = ffn_backward(grad_one, first, kept_first, pipe, "ffn1", pieces, True)
    names, shapes, full = first_grads["gathered"]
    grad_zero, full = pipe.tie(grad_zero, full)
    gathered = dict(zip(names, unstack_pieces(full, shapes)))
    late = [
        first_grads["bias"],
        first_grads["out_bias"],
        first_grads["gain"],
        first_grads["shift"],
    ]
    pipe.start("late", total_steps(late))
    (input_grad,) = exchange([grad_zero.astype(BF16)], device_count, False, 6, True)
    input_grad = pipe.tie(input_grad)
    results = pipe.finish()
    early = results["early"]
    late = results["late"]
    qkv_grad = results["qkv"]
    if "rest" in gathered:
        glu_grad, out_grads = gathered["rest"][:glu_height], gathered["rest"][glu_height:]
    else:
        glu_grad, out_grads = gathered["glu"], gathered["outs"]
    attn_out_grad, conv_out_grad = out_grads[:out_height], out_grads[out_height:]
    piece = D // device_count
    piece_start = (lax.axis_index("row") * col_size + lax.axis_index("col")) * piece
    own = lambda vector: lax.dynamic_slice_in_dim(vector, piece_start, piece, 0)
    qkv_width = qkv_grad.shape[1] // 3
    glu_width = glu_grad.shape[1] // 2
    return (
        output,
        to_float(input_grad),
        own(late[2]),
        own(late[3]),
        results["ffn1_in"],
        late[0],
        results["ffn1_out"],
        own(late[1]),
        own(early[15]),
        own(early[16]),
        qkv_grad[:, :qkv_width],
        early[13],
        qkv_grad[:, qkv_width : 2 * qkv_width],
        qkv_grad[:, 2 * qkv_width :],
        early[14],
        early[12].reshape(-1, HEAD)[:BUCKETS],
        attn_out_grad,
        own(early[11]),
        own(early[9]),
        own(early[10]),
        glu_grad[:, :glu_width],
        glu_grad[:, glu_width:],
        early[1].reshape(KERNEL, D),
        early[2],
        early[3],
        conv_out_grad,
        own(early[6]),
        own(early[7]),
        gathered["ffn2_in"],
        early[0],
        gathered["ffn2_out"],
        own(early[8]),
        own(early[4]),
        own(early[5]),
    )


def solution(mesh):
    in_specs = (
        P("dp", ("row", "col")),
        P("dp"),
        P("dp", ("row", "col")),
        P(("row", "col")),
        P(("row", "col")),
        P("row", "col"),
        P(),
        P("col", "row"),
        P(("row", "col")),
        P(("row", "col")),
        P(("row", "col")),
        P("row", "col"),
        P(),
        P("row", "col"),
        P("row", "col"),
        P(),
        P(),
        P("col", "row"),
        P(("row", "col")),
        P(("row", "col")),
        P(("row", "col")),
        P("row", "col"),
        P("row", "col"),
        P(),
        P(),
        P(),
        P("col", "row"),
        P(("row", "col")),
        P(("row", "col")),
        P("row", "col"),
        P(),
        P("col", "row"),
        P(("row", "col")),
        P(("row", "col")),
        P(("row", "col")),
    )
    out_specs = (
        P("dp", ("row", "col")),
        P("dp", ("row", "col")),
        P(("row", "col")),
        P(("row", "col")),
        P("row", "col"),
        P(),
        P("col", "row"),
        P(("row", "col")),
        P(("row", "col")),
        P(("row", "col")),
        P("row", "col"),
        P(),
        P("row", "col"),
        P("row", "col"),
        P(),
        P(),
        P("col", "row"),
        P(("row", "col")),
        P(("row", "col")),
        P(("row", "col")),
        P("row", "col"),
        P("row", "col"),
        P(),
        P(),
        P(),
        P("col", "row"),
        P(("row", "col")),
        P(("row", "col")),
        P("row", "col"),
        P(),
        P("col", "row"),
        P(("row", "col")),
        P(("row", "col")),
        P(("row", "col")),
    )
    return jax.shard_map(local, mesh=mesh, in_specs=in_specs, out_specs=out_specs, check_vma=False)
```
